8 devices in a mesh: rep: 1 (over z), dp: 8 (over x, y, core).
Axes of the slice: x: 2, y: 2, z: 1, core: 2. Of those that a mesh axis runs over, the one named last changes fastest.
Arguments:
- g_w_gate: bfloat16 [8, 2, 1024, 4096], P(('rep', 'dp'))
- g_w_up: bfloat16 [8, 2, 1024, 4096], P(('rep', 'dp'))
- g_w_down: bfloat16 [8, 2, 4096, 1024], P(('rep', 'dp'))
- w_gate: bfloat16 [2, 1024, 4096], replicated
- w_up: bfloat16 [2, 1024, 4096], replicated
- w_down: bfloat16 [2, 4096, 1024], replicated
- m_w_gate: float32 [2, 1024, 4096], P(None, 'dp')
- m_w_up: float32 [2, 1024, 4096], P(None, 'dp')
- m_w_down: float32 [2, 4096, 1024], P(None, 'dp')
- v_w_gate: float32 [2, 1024, 4096], P(None, 'dp')
- v_w_up: float32 [2, 1024, 4096], P(None, 'dp')
- v_w_down: float32 [2, 4096, 1024], P(None, 'dp')
Outputs:
- output 1: bfloat16 [2, 1024, 4096], P('rep')
- output 2: bfloat16 [2, 1024, 4096], P('rep')
- output 3: bfloat16 [2, 4096, 1024], P('rep')
- output 4: float32 [2, 1024, 4096], P('rep', 'dp')
- output 5: float32 [2, 1024, 4096], P('rep', 'dp')
- output 6: float32 [2, 4096, 1024], P('rep', 'dp')
- output 7: float32 [2, 1024, 4096], P('rep', 'dp')
- output 8: float32 [2, 1024, 4096], P('rep', 'dp')
- output 9: float32 [2, 4096, 1024], P('rep', 'dp')
All inputs are finite; a program needn't handle non-finite values.
Results may differ from the reference program's by a relative error of at most 0.022.
Values are sent between devices in bfloat16 or wider.
A program may use at most 2 GiB of HBM per device.

```python
import jax
import jax.numpy as jnp
from jax import lax

DEVICES = 8
D = 1024
FF = 4096
LAYERS = 2
NAMES = ("w_gate", "w_up", "w_down")
SHAPES = {"w_gate": (LAYERS, D, FF), "w_up": (LAYERS, D, FF), "w_down": (LAYERS, FF, D)}


def setup_inputs(seed: int = 0, part: int = 0) -> dict:
    kz, *keys = jax.random.split(jax.random.key(seed), 1 + 5 * len(NAMES))
    loud = 2.0 ** jax.random.uniform(kz, (), jnp.float32, -1.0, 1.0)
    drawn = {}
    for name, key, both in zip(NAMES, keys[:3], keys[3:6], strict=True):
        own = jax.random.normal(jax.random.fold_in(key, part), (DEVICES, *SHAPES[name]), jnp.float32)
        shared = jax.random.normal(jax.random.fold_in(both, part), SHAPES[name], jnp.float32)
        drawn["g_" + name] = (loud * (0.7 * shared / DEVICES + 0.7 * own * DEVICES**-0.5)).astype(jnp.bfloat16)
    for name, key in zip(NAMES, keys[6:9], strict=True):
        drawn[name] = (jax.random.normal(key, SHAPES[name], jnp.float32) * SHAPES[name][1] ** -0.5).astype(jnp.bfloat16)
    for name, key in zip(NAMES, keys[9:12], strict=True):
        drawn["m_" + name] = loud * 0.5 * jax.random.normal(key, SHAPES[name], jnp.float32)
    for name, key in zip(NAMES, keys[12:15], strict=True):
        drawn["v_" + name] = loud * loud * jax.random.uniform(key, SHAPES[name], jnp.float32, 0.5, 1.5)
    return drawn


def adamw(w, m, v, g):
    m = 0.9 * m + 0.1 * g
    v = 0.95 * v + 0.05 * g * g
    step = m * lax.rsqrt(v + 1e-8) + 0.1 * w
    return (w - 0.02 * step).astype(jnp.bfloat16), m, v


def clipped(gradients, sum_of_squares, count):
    factor = jnp.minimum(1.0, 0.5 * lax.rsqrt(sum_of_squares / count + 1e-30))
    return [g * factor for g in gradients]


def reference(g_w_gate, g_w_up, g_w_down, w_gate, w_up, w_down, m_w_gate, m_w_up, m_w_down, v_w_gate, v_w_up, v_w_down):
    def total(terms):
        return lax.scan(lambda so_far, term: (so_far + term.astype(jnp.float32), None), jnp.zeros(terms.shape[1:], jnp.float32), terms)[0]

    gradients = [total(terms).astype(jnp.bfloat16).astype(jnp.float32) for terms in (g_w_gate, g_w_up, g_w_down)]
    gradients = clipped(gradients, sum(jnp.sum(g * g) for g in gradients), sum(g.size for g in gradients))
    new = [
        adamw(w.astype(jnp.float32), m, v, g)
        for w, m, v, g in zip((w_gate, w_up, w_down), (m_w_gate, m_w_up, m_w_down), (v_w_gate, v_w_up, v_w_down), gradients, strict=True)
    ]
    return tuple(one[which] for which in range(3) for one in new)
```

```python
import functools

import jax
import jax.numpy as jnp
from jax import lax
from jax.experimental import pallas as pl
from jax.experimental.pallas import tpu as pltpu
from jax.sharding import PartitionSpec as P

BF, F32 = jnp.bfloat16, jnp.float32
RING = 4
FEED = 2
ME, XN, YN, DG = range(4)
XD, XO, XT, YD, YO, YT = range(6)


def moments(m, v, g):
    return 0.9 * m + 0.1 * g, 0.95 * v + 0.05 * g * g


def kernel(*refs, n, layers, count):
    it = iter(refs)
    take = lambda k: [next(it) for _ in range(k)]
    g, w, m, v = take(3), take(3), take(3), take(3)
    whole, gsum, factor_ref = take(3), take(3), next(it)
    pair, land = take(3), take(3)
    gring, mring, vring, wring = take(2), take(2), take(2), take(2)
    squares, factor_v = take(2)
    d2d_s, d2d_r, lk_s, lk_r, ring_s, feed_s = take(6)
    sq_s, sq_r, own_s, own_r, fwd_s, fwd_r, rel_s, rel_r, loc_s = take(9)

    me = lax.axis_index("dp")
    core, chip = me % 2, me // 2
    cy, cx = chip % 2, chip // 2
    at = lambda x, y, c: 4 * x + 2 * y + c
    mate = at(cx, cy, 1 - core)
    xnbr, ynbr = at(1 - cx, cy, core), at(cx, 1 - cy, core)
    owners = [lambda c: at(cx, cy, c), lambda c: at(1 - cx, cy, c), lambda c: at(cx, 1 - cy, c), lambda c: at(1 - cx, 1 - cy, c)]

    def remote(src, dst, s, r, device):
        return pltpu.make_async_remote_copy(
            src_ref=src, dst_ref=dst, send_sem=s, recv_sem=r, device_id={"dp": device}, device_id_type=pl.DeviceIdType.MESH
        )

    barrier = pltpu.get_barrier_semaphore()
    for k in range(1, n):
        pl.semaphore_signal(barrier, inc=1, device_id={"dp": (me + k) % n}, device_id_type=pl.DeviceIdType.MESH)
    pl.semaphore_wait(barrier, n - 1)

    units = [(i, layer) for i in range(3) for layer in range(layers)]
    kind = [0, 0, 1]
    half = [pair[i].shape[3] for i in range(3)]

    def rows(i, device, h):
        return pl.ds(pl.multiple_of(device * (2 * half[i]) + h * half[i], half[i]), half[i])

    steps = []
    for u in range(len(units)):
        steps += [("send", DG, u, 0, XD, None), ("send", DG, u, 1, YD, None)]
    for u in range(len(units)):
        steps += [("send", XN, u, 0, XO, None), ("send", YN, u, 1, YO, None)]
    for u in range(len(units)):
        steps += [("send", YN, u, 0, YT, XD), ("send", XN, u, 1, XT, YD)]
    for u in range(len(units)):
        steps += [("sum", ME, u, 0, XO, YT), ("sum", ME, u, 1, YO, XT)]

    def exchange(step):
        _, block, u, h, _, _ = step
        i, layer = units[u]
        return remote(
            g[i].at[0, layer, rows(i, owners[block](1 - core), h)], pair[i].at[block, layer, h], d2d_s.at[block, u, h], d2d_r.at[block, u, h], mate
        )

    order = {0: [], 1: []}
    for k, step in enumerate(steps):
        order[kind[units[step[2]][0]]].append(k)
    place = {k: (c, p) for c in order for p, k in enumerate(order[c])}

    def term(k):
        _, block, u, h, _, _ = steps[k]
        i, layer = units[u]
        c, p = place[k]
        slot = p % RING
        return pltpu.make_async_copy(g[i].at[0, layer, rows(i, owners[block](core), h)], gring[c].at[slot], ring_s.at[c, slot])

    def push(step):
        _, block, u, h, stream, _ = step
        i, layer = units[u]
        return remote(pair[i].at[block, layer, h], land[i].at[stream, layer], lk_s.at[stream, u], lk_r.at[stream, u], xnbr if stream < YD else ynbr)

    def arrived(stream, u):
        i, layer = units[u]
        return remote(land[i].at[stream, layer], land[i].at[stream, layer], lk_s.at[stream, u], lk_r.at[stream, u], xnbr if stream < YD else ynbr)

    ahead = 12
    exchanged, started = 0, {0: 0, 1: 0}

    def next_exchange():
        nonlocal exchanged
        if exchanged < len(steps):
            exchange(steps[exchanged]).start()
            exchanged += 1

    def next_term(c):
        if started[c] < len(order[c]):
            term(order[c][started[c]]).start()
            started[c] += 1

    next_exchange()
    next_exchange()
    for _ in range(RING):
        next_term(0)
    for _ in range(ahead - 2):
        next_exchange()
    for _ in range(RING):
        next_term(1)

    def feed(u, h, k):
        i, layer = units[u]
        c, slot = kind[i], k % FEED
        mine = pl.ds(h * half[i], half[i])
        return [
            pltpu.make_async_copy(m[i].at[layer, mine], mring[c].at[slot], feed_s.at[0, c, slot]),
            pltpu.make_async_copy(v[i].at[layer, mine], vring[c].at[slot], feed_s.at[1, c, slot]),
            pltpu.make_async_copy(w[i].at[layer, rows(i, me, h)], wring[c].at[slot], feed_s.at[2, c, slot]),
        ]

    fed = [(u, h) for u in range(len(units)) for h in range(2)]
    feed_order = {c: [k for k, (u, h) in enumerate(fed) if kind[units[u][0]] == c] for c in (0, 1)}
    feed_at = {k: p for c in (0, 1) for p, k in enumerate(feed_order[c])}
    for c in (0, 1):
        for k in feed_order[c][:FEED]:
            for copy in feed(*fed[k], feed_at[k]):
                copy.start()

    zero = jnp.zeros((8, 128), F32)
    total = (zero,) * 4
    for k, step in enumerate(steps):
        what, block, u, h, stream, other = step
        i, layer = units[u]
        c, p = place[k]
        exchange_in = remote(pair[i].at[block, layer, h], pair[i].at[block, layer, h], d2d_s.at[block, u, h], d2d_r.at[block, u, h], mate)
        exchange_in.wait_recv()
        term(k).wait()
        more = []
        if what == "sum":
            arrived(stream, u).wait_recv()
            more.append(land[i].at[stream, layer])
        if other is not None:
            arrived(other, u).wait_recv()
            more.append(land[i].at[other, layer])
        dst, own = pair[i].at[block, layer, h], gring[c].at[p % RING]
        cols = dst.shape[1]
        tile = 65536 // cols

        def body(r, acc, dst=dst, own=own, more=more, cols=cols, tile=tile, what=what):
            at_rows = pl.ds(pl.multiple_of(r * tile, tile), tile)
            s = own[at_rows, :].astype(F32) + dst[at_rows, :].astype(F32)
            for one in more:
                s = s + one[at_rows, :].astype(F32)
            b = s.astype(BF)
            dst[at_rows, :] = b
            if what == "sum":
                q = b.astype(F32)
                q = q * q
                acc = list(acc)
                for a in range(tile // 8):
                    for z in range(cols // 128):
                        acc[(a + z) % 4] = acc[(a + z) % 4] + q[8 * a : 8 * a + 8, 128 * z : 128 * z + 128]
                acc = tuple(acc)
            return acc

        done = lax.fori_loop(0, half[i] // tile, body, total if what == "sum" else ())
        total = done if what == "sum" else total
        next_term(c)
        next_exchange()
        if what == "send":
            push(step).start()
        else:
            pltpu.make_async_copy(dst, gsum[i].at[layer, pl.ds(h * half[i], half[i])], loc_s.at[0, u, h]).start()

    squares[n] = total[0] + total[1] + total[2] + total[3]
    for k in range(1, n):
        remote(squares.at[n], squares.at[me], sq_s.at[k], sq_r.at[me], (me + k) % n).start()
    for step in steps:
        exchange(step).wait_send()
        if step[0] == "send":
            push(step).wait_send()
    squares[me] = squares[n]
    for k in range(1, n):
        remote(squares.at[n], squares.at[(me + k) % n], sq_s.at[k], sq_r.at[(me + k) % n], (me + k) % n).wait_recv()
    everything = squares[0]
    for k in range(1, n):
        everything = everything + squares[k]
    everything = jnp.sum(jnp.sum(everything, axis=0, keepdims=True), axis=1, keepdims=True)
    factor = jnp.minimum(1.0, 0.5 * lax.rsqrt(everything / count + 1e-30))
    factor_v[...] = jnp.broadcast_to(factor, (8, 128))

    def out(i, layer, device, h):
        return whole[i].at[layer, rows(i, device, h)]

    def own_copies(u, h):
        i, layer = units[u]
        src = pair[i].at[DG, layer, h]
        dst = out(i, layer, me, h)
        return [
            functools.partial(remote, src, dst, own_s.at[0, u, h], own_r.at[0, u, h], xnbr),
            functools.partial(remote, src, dst, own_s.at[1, u, h], own_r.at[1, u, h], ynbr),
            functools.partial(remote, src, dst, rel_s.at[ME, u, h], rel_r.at[ME, u, h], mate),
            functools.partial(pltpu.make_async_copy, src, dst, loc_s.at[1, u, h]),
        ]

    for k, (u, h) in enumerate(fed):
        i, layer = units[u]
        c, slot = kind[i], feed_at[k] % FEED
        for copy in feed(u, h, feed_at[k]):
            copy.wait()
        dst, src, mm, vv, ww = pair[i].at[DG, layer, h], pair[i].at[ME, layer, h], mring[c].at[slot], vring[c].at[slot], wring[c].at[slot]
        cols = dst.shape[1]
        tile = 32768 // cols if cols < 4096 else 16

        def body(r, _, dst=dst, src=src, mm=mm, vv=vv, ww=ww, tile=tile):
            at_rows = pl.ds(pl.multiple_of(r * tile, tile), tile)
            grad = src[at_rows, :].astype(F32) * factor_v[0:1, 0:1]
            m_new, v_new = moments(mm[at_rows, :], vv[at_rows, :], grad)
            weight = ww[at_rows, :].astype(F32)
            dst[at_rows, :] = (weight - 0.02 * (m_new * lax.rsqrt(v_new + 1e-8) + 0.1 * weight)).astype(BF)
            return 0

        lax.fori_loop(0, half[i] // tile, body, 0)
        if feed_at[k] + FEED < len(feed_order[c]):
            later = feed_order[c][feed_at[k] + FEED]
            for copy in feed(*fed[later], feed_at[later]):
                copy.start()
        for copy in own_copies(u, h):
            copy().start()

    started_late = []

    def relay(u, h, block):
        i, layer = units[u]
        here = out(i, layer, owners[block](core), h)
        copy = remote(here, here, rel_s.at[block, u, h], rel_r.at[block, u, h], mate)
        copy.start()
        started_late.append(copy)

    def onward(u, h, block, to, device):
        i, layer = units[u]
        here = out(i, layer, owners[block](core), h)
        copy = remote(here, here, fwd_s.at[to, u], fwd_r.at[to, u], device)
        copy.start()
        started_late.append(copy)

    def from_link(u, h, which):
        i, layer = units[u]
        there = out(i, layer, owners[(XN, YN)[which]](core), h)
        remote(there, there, own_s.at[which, u, h], own_r.at[which, u, h], (xnbr, ynbr)[which]).wait_recv()

    for u in range(len(units)):
        from_link(u, 0, 0)
        onward(u, 0, XN, 1, ynbr)
        relay(u, 0, XN)
        from_link(u, 0, 1)
        relay(u, 0, YN)
        from_link(u, 1, 1)
        onward(u, 1, YN, 0, xnbr)
        relay(u, 1, YN)
        from_link(u, 1, 0)
        relay(u, 1, XN)
    for u in range(len(units)):
        i, layer = units[u]
        for h, to, device in ((0, 1, ynbr), (1, 0, xnbr)):
            there = out(i, layer, owners[DG](core), h)
            remote(there, there, fwd_s.at[to, u], fwd_r.at[to, u], device).wait_recv()
            relay(u, h, DG)

    for copy in started_late:
        copy.wait_send()
    for u, h in fed:
        i, layer = units[u]
        for copy in own_copies(u, h)[:3]:
            copy().wait_send()
        own_copies(u, h)[3]().wait()
        pltpu.make_async_copy(pair[i].at[ME, layer, h], gsum[i].at[layer, pl.ds(h * half[i], half[i])], loc_s.at[0, u, h]).wait()
        for block in range(4):
            there = out(i, layer, owners[block](1 - core), h)
            remote(there, there, rel_s.at[block, u, h], rel_r.at[block, u, h], mate).wait_recv()
    for k in range(1, n):
        remote(squares.at[n], squares.at[me], sq_s.at[k], sq_r.at[me], (me + k) % n).wait_send()
    done = pltpu.make_async_copy(factor_v, factor_ref, loc_s.at[0, 0, 0])
    done.start()
    done.wait()


def solution(mesh):
    n = mesh.shape["dp"]

    def step(*arrays):
        terms, weights, m, v = (arrays[i : i + 3] for i in (0, 3, 6, 9))
        layers = weights[0].shape[0]
        blocks = [(one.shape[1] // 2, one.shape[2]) for one in m]
        kinds = (blocks[0], blocks[2])
        count = float(n * sum(one.size for one in m))
        dma = pltpu.SemaphoreType.DMA
        units = 3 * layers
        any_space = pl.BlockSpec(memory_space=pl.ANY)
        out = pl.pallas_call(
            functools.partial(kernel, n=n, layers=layers, count=count),
            name="step",
            out_shape=[jax.ShapeDtypeStruct(one.shape, BF) for one in weights]
            + [jax.ShapeDtypeStruct(one.shape, BF) for one in m]
            + [jax.ShapeDtypeStruct((8, 128), F32)],
            in_specs=[any_space] * 12,
            out_specs=[any_space] * 7,
            scratch_shapes=[pltpu.VMEM((4, layers, 2, *b), BF) for b in blocks]
            + [pltpu.VMEM((6, layers, *b), BF) for b in blocks]
            + [pltpu.VMEM((RING, *b), BF) for b in kinds]
            + [pltpu.VMEM((FEED, *b), F32) for b in kinds] * 2
            + [pltpu.VMEM((FEED, *b), BF) for b in kinds]
            + [pltpu.VMEM((n + 1, 8, 128), F32), pltpu.VMEM((8, 128), F32)]
            + [dma((4, units, 2)), dma((4, units, 2)), dma((6, units)), dma((6, units)), dma((2, RING)), dma((3, 2, FEED))]
            + [dma((n,)), dma((n,)), dma((2, units, 2)), dma((2, units, 2)), dma((2, units)), dma((2, units))]
            + [dma((4, units, 2)), dma((4, units, 2)), dma((2, units, 2))],
            compiler_params=pltpu.CompilerParams(collective_id=0, has_side_effects=True, vmem_limit_bytes=62 * 2**20),
        )(*terms, *weights, *m, *v)
        whole, sums, factor = out[:3], out[3:6], out[6][0, 0]
        new = [moments(a, b, s.astype(F32) * factor) for a, b, s in zip(m, v, sums, strict=True)]
        return (*whole, *(one[0] for one in new), *(one[1] for one in new))

    all_of, cut = P(None, None, None), P(None, "dp", None)
    return jax.shard_map(
        step,
        mesh=mesh,
        in_specs=(P(("rep", "dp"), None, None, None),) * 3 + (all_of,) * 3 + (cut,) * 6,
        out_specs=(P("rep", None, None),) * 3 + (P("rep", "dp", None),) * 6,
        check_vma=False,
    )
```

```python
import functools

import jax
import jax.numpy as jnp
from jax import lax
from jax.experimental import pallas as pl
from jax.experimental.pallas import tpu as pltpu
from jax.sharding import PartitionSpec as P


BF, F32 = jnp.bfloat16, jnp.float32
RING = 4
FEED = 2
KEPT = 2
ME, XN, YN, DG = range(4)
XD, XO, XT, YD, YO, YT = range(6)


def moments(m, v, g):
    return 0.9 * m + 0.1 * g, 0.95 * v + 0.05 * g * g


def kernel(*refs, n, layers, count):
    it = iter(refs)
    take = lambda k: [next(it) for _ in range(k)]
    g, w, m, v = take(3), take(3), take(3), take(3)
    whole, ends, gsum, factor_ref = take(KEPT), take(2), take(3), next(it)
    pair, land = take(3), take(3)
    gring, mring, vring, wring = take(2), take(2), take(2), take(2)
    squares, factor_v = take(2)
    d2d_s, d2d_r, lk_s, lk_r, ring_s, feed_s = take(6)
    sq_s, sq_r, own_s, own_r, fwd_s, fwd_r, rel_s, rel_r, loc_s = take(9)

    me = lax.axis_index("dp")
    core, chip = me % 2, me // 2
    cy, cx = chip % 2, chip // 2
    at = lambda x, y, c: 4 * x + 2 * y + c
    mate = at(cx, cy, 1 - core)
    xnbr, ynbr = at(1 - cx, cy, core), at(cx, 1 - cy, core)
    owners = [lambda c: at(cx, cy, c), lambda c: at(1 - cx, cy, c), lambda c: at(cx, 1 - cy, c), lambda c: at(1 - cx, 1 - cy, c)]

    def remote(src, dst, s, r, device):
        return pltpu.make_async_remote_copy(
            src_ref=src, dst_ref=dst, send_sem=s, recv_sem=r, device_id={"dp": device}, device_id_type=pl.DeviceIdType.MESH
        )

    barrier = pltpu.get_barrier_semaphore()
    for k in range(1, n):
        pl.semaphore_signal(barrier, inc=1, device_id={"dp": (me + k) % n}, device_id_type=pl.DeviceIdType.MESH)
    pl.semaphore_wait(barrier, n - 1)

    units = [(i, layer) for i in range(3) for layer in range(layers)]
    kind = [0, 0, 1]
    half = [pair[i].shape[3] for i in range(3)]

    def rows(i, device, h):
        return pl.ds(pl.multiple_of(device * (2 * half[i]) + h * half[i], half[i]), half[i])

    steps = []
    for u in range(len(units)):
        steps += [("send", DG, u, 0, XD, None), ("send", DG, u, 1, YD, None)]
    for u in range(len(units)):
        steps += [("send", XN, u, 0, XO, None), ("send", YN, u, 1, YO, None)]
    for u in range(len(units)):
        steps += [("send", YN, u, 0, YT, XD), ("send", XN, u, 1, XT, YD)]
    for u in range(len(units)):
        steps += [("sum", ME, u, 0, XO, YT), ("sum", ME, u, 1, YO, XT)]

    def exchange(step):
        _, block, u, h, _, _ = step
        i, layer = units[u]
        return remote(
            g[i].at[0, layer, rows(i, owners[block](1 - core), h)], pair[i].at[block, layer, h], d2d_s.at[block, u, h], d2d_r.at[block, u, h], mate
        )

    order = {0: [], 1: []}
    for k, step in enumerate(steps):
        order[kind[units[step[2]][0]]].append(k)
    place = {k: (c, p) for c in order for p, k in enumerate(order[c])}

    def term(k):
        _, block, u, h, _, _ = steps[k]
        i, layer = units[u]
        c, p = place[k]
        slot = p % RING
        return pltpu.make_async_copy(g[i].at[0, layer, rows(i, owners[block](core), h)], gring[c].at[slot], ring_s.at[c, slot])

    def push(step):
        _, block, u, h, stream, _ = step
        i, layer = units[u]
        return remote(pair[i].at[block, layer, h], land[i].at[stream, layer], lk_s.at[stream, u], lk_r.at[stream, u], xnbr if stream < YD else ynbr)

    def arrived(stream, u):
        i, layer = units[u]
        return remote(land[i].at[stream, layer], land[i].at[stream, layer], lk_s.at[stream, u], lk_r.at[stream, u], xnbr if stream < YD else ynbr)

    ahead = 12
    exchanged, started = 0, {0: 0, 1: 0}

    def next_exchange():
        nonlocal exchanged
        if exchanged < len(steps):
            exchange(steps[exchanged]).start()
            exchanged += 1

    def next_term(c):
        if started[c] < len(order[c]):
            term(order[c][started[c]]).start()
            started[c] += 1

    next_exchange()
    next_exchange()
    for _ in range(RING):
        next_term(0)
    for _ in range(ahead - 2):
        next_exchange()
    for _ in range(RING):
        next_term(1)

    def feed(u, h, k):
        i, layer = units[u]
        c, slot = kind[i], k % FEED
        mine = pl.ds(h * half[i], half[i])
        return [
            pltpu.make_async_copy(m[i].at[layer, mine], mring[c].at[slot], feed_s.at[0, c, slot]),
            pltpu.make_async_copy(v[i].at[layer, mine], vring[c].at[slot], feed_s.at[1, c, slot]),
            pltpu.make_async_copy(w[i].at[layer, rows(i, me, h)], wring[c].at[slot], feed_s.at[2, c, slot]),
        ]

    fed = [(u, h) for u in range(len(units)) for h in range(2)]
    feed_order = {c: [k for k, (u, h) in enumerate(fed) if kind[units[u][0]] == c] for c in (0, 1)}
    feed_at = {k: p for c in (0, 1) for p, k in enumerate(feed_order[c])}
    for c in (0, 1):
        for k in feed_order[c][:FEED]:
            for copy in feed(*fed[k], feed_at[k]):
                copy.start()

    zero = jnp.zeros((8, 128), F32)
    total = (zero,) * 4
    for k, step in enumerate(steps):
        what, block, u, h, stream, other = step
        i, layer = units[u]
        c, p = place[k]
        exchange_in = remote(pair[i].at[block, layer, h], pair[i].at[block, layer, h], d2d_s.at[block, u, h], d2d_r.at[block, u, h], mate)
        exchange_in.wait_recv()
        term(k).wait()
        more = []
        if what == "sum":
            arrived(stream, u).wait_recv()
            more.append(land[i].at[stream, layer])
        if other is not None:
            arrived(other, u).wait_recv()
            more.append(land[i].at[other, layer])
        dst, own = pair[i].at[block, layer, h], gring[c].at[p % RING]
        cols = dst.shape[1]
        tile = 65536 // cols

        def body(r, acc, dst=dst, own=own, more=more, cols=cols, tile=tile, what=what):
            at_rows = pl.ds(pl.multiple_of(r * tile, tile), tile)
            s = own[at_rows, :].astype(F32) + dst[at_rows, :].astype(F32)
            for one in more:
                s = s + one[at_rows, :].astype(F32)
            b = s.astype(BF)
            dst[at_rows, :] = b
            if what == "sum":
                q = b.astype(F32)
                q = q * q
                acc = list(acc)
                for a in range(tile // 8):
                    for z in range(cols // 128):
                        acc[(a + z) % 4] = acc[(a + z) % 4] + q[8 * a : 8 * a + 8, 128 * z : 128 * z + 128]
                acc = tuple(acc)
            return acc

        done = lax.fori_loop(0, half[i] // tile, body, total if what == "sum" else ())
        total = done if what == "sum" else total
        next_term(c)
        next_exchange()
        if what == "send":
            push(step).start()
        else:
            pltpu.make_async_copy(dst, gsum[i].at[layer, pl.ds(h * half[i], half[i])], loc_s.at[0, u, h]).start()

    squares[n] = total[0] + total[1] + total[2] + total[3]
    for k in range(1, n):
        remote(squares.at[n], squares.at[me], sq_s.at[k], sq_r.at[me], (me + k) % n).start()
    for step in steps:
        exchange(step).wait_send()
        if step[0] == "send":
            push(step).wait_send()
    squares[me] = squares[n]
    for k in range(1, n):
        remote(squares.at[n], squares.at[(me + k) % n], sq_s.at[k], sq_r.at[(me + k) % n], (me + k) % n).wait_recv()
    everything = squares[0]
    for k in range(1, n):
        everything = everything + squares[k]
    everything = jnp.sum(jnp.sum(everything, axis=0, keepdims=True), axis=1, keepdims=True)
    factor = jnp.minimum(1.0, 0.5 * lax.rsqrt(everything / count + 1e-30))
    factor_v[...] = jnp.broadcast_to(factor, (8, 128))

    def out(i, layer, device, h):
        return whole[i].at[layer, rows(i, device, h)]

    def own_copies(u, h):
        i, layer = units[u]
        src = pair[i].at[DG, layer, h]
        if i >= KEPT:
            return [functools.partial(pltpu.make_async_copy, src, ends[h].at[layer], loc_s.at[1, u, h])]
        dst = out(i, layer, me, h)
        return [
            functools.partial(pltpu.make_async_copy, src, dst, loc_s.at[1, u, h]),
            functools.partial(remote, src, dst, own_s.at[0, u, h], own_r.at[0, u, h], xnbr),
            functools.partial(remote, src, dst, own_s.at[1, u, h], own_r.at[1, u, h], ynbr),
            functools.partial(remote, src, dst, rel_s.at[ME, u, h], rel_r.at[ME, u, h], mate),
        ]

    for k, (u, h) in enumerate(fed):
        i, layer = units[u]
        c, slot = kind[i], feed_at[k] % FEED
        for copy in feed(u, h, feed_at[k]):
            copy.wait()
        dst, src, mm, vv, ww = pair[i].at[DG, layer, h], pair[i].at[ME, layer, h], mring[c].at[slot], vring[c].at[slot], wring[c].at[slot]
        cols = dst.shape[1]
        tile = 32768 // cols if cols < 4096 else 16

        def body(r, _, dst=dst, src=src, mm=mm, vv=vv, ww=ww, tile=tile):
            at_rows = pl.ds(pl.multiple_of(r * tile, tile), tile)
            grad = src[at_rows, :].astype(F32) * factor_v[0:1, 0:1]
            m_new, v_new = moments(mm[at_rows, :], vv[at_rows, :], grad)
            weight = ww[at_rows, :].astype(F32)
            dst[at_rows, :] = (weight - 0.02 * (m_new * lax.rsqrt(v_new + 1e-8) + 0.1 * weight)).astype(BF)
            return 0

        lax.fori_loop(0, half[i] // tile, body, 0)
        if feed_at[k] + FEED < len(feed_order[c]):
            later = feed_order[c][feed_at[k] + FEED]
            for copy in feed(*fed[later], feed_at[later]):
                copy.start()
        for copy in own_copies(u, h):
            copy().start()

    started_late = []

    def relay(u, h, block):
        i, layer = units[u]
        here = out(i, layer, owners[block](core), h)
        copy = remote(here, here, rel_s.at[block, u, h], rel_r.at[block, u, h], mate)
        copy.start()
        started_late.append(copy)

    def onward(u, h, block, to, device):
        i, layer = units[u]
        here = out(i, layer, owners[block](core), h)
        copy = remote(here, here, fwd_s.at[to, u], fwd_r.at[to, u], device)
        copy.start()
        started_late.append(copy)

    def from_link(u, h, which):
        i, layer = units[u]
        there = out(i, layer, owners[(XN, YN)[which]](core), h)
        remote(there, there, own_s.at[which, u, h], own_r.at[which, u, h], (xnbr, ynbr)[which]).wait_recv()

    gathered = [u for u in range(len(units)) if units[u][0] < KEPT]
    for u in gathered:
        from_link(u, 0, 0)
        onward(u, 0, XN, 1, ynbr)
        relay(u, 0, XN)
        from_link(u, 0, 1)
        relay(u, 0, YN)
        from_link(u, 1, 1)
        onward(u, 1, YN, 0, xnbr)
        relay(u, 1, YN)
        from_link(u, 1, 0)
        relay(u, 1, XN)
    for u in gathered:
        i, layer = units[u]
        for h, to, device in ((0, 1, ynbr), (1, 0, xnbr)):
            there = out(i, layer, owners[DG](core), h)
            remote(there, there, fwd_s.at[to, u], fwd_r.at[to, u], device).wait_recv()
            relay(u, h, DG)

    for copy in started_late:
        copy.wait_send()
    for u, h in fed:
        i, layer = units[u]
        own_copies(u, h)[0]().wait()
        for copy in own_copies(u, h)[1:]:
            copy().wait_send()
        pltpu.make_async_copy(pair[i].at[ME, layer, h], gsum[i].at[layer, pl.ds(h * half[i], half[i])], loc_s.at[0, u, h]).wait()
        for block in range(4) if i < KEPT else ():
            there = out(i, layer, owners[block](1 - core), h)
            remote(there, there, rel_s.at[block, u, h], rel_r.at[block, u, h], mate).wait_recv()
    for k in range(1, n):
        remote(squares.at[n], squares.at[me], sq_s.at[k], sq_r.at[me], (me + k) % n).wait_send()
    done = pltpu.make_async_copy(factor_v, factor_ref, loc_s.at[0, 0, 0])
    done.start()
    done.wait()


def move_kernel(*refs, parts):
    k = (len(refs) - 3) // 2
    src, dst, (buf, in_s, out_s) = refs[:k], refs[k : 2 * k], refs[2 * k :]
    pieces = []
    for a in range(k):
        layers, height = src[a].shape[:2]
        size = height // parts
        pieces += [(a, layer, pl.ds(p * size, size)) for layer in range(layers) for p in range(parts)]
    load = lambda z: pltpu.make_async_copy(src[pieces[z][0]].at[pieces[z][1], pieces[z][2]], buf.at[z], in_s.at[z])
    store = lambda z: pltpu.make_async_copy(buf.at[z], dst[pieces[z][0]].at[pieces[z][1], pieces[z][2]], out_s.at[z])
    for z in range(len(pieces)):
        load(z).start()
    for z in range(len(pieces)):
        load(z).wait()
        store(z).start()
    for z in range(len(pieces)):
        store(z).wait()


def move(*arrays, parts=4):
    layers, height, width = arrays[0].shape
    pieces = len(arrays) * layers * parts
    size = sum(a.size * 4 for a in arrays)
    return pl.pallas_call(
        functools.partial(move_kernel, parts=parts),
        name="move",
        out_shape=[jax.ShapeDtypeStruct(a.shape, a.dtype) for a in arrays],
        in_specs=[pl.BlockSpec(memory_space=pl.ANY)] * len(arrays),
        out_specs=[pl.BlockSpec(memory_space=pl.ANY)] * len(arrays),
        scratch_shapes=[
            pltpu.VMEM((pieces, height // parts, width), arrays[0].dtype),
            pltpu.SemaphoreType.DMA((pieces,)),
            pltpu.SemaphoreType.DMA((pieces,)),
        ],
        compiler_params=pltpu.CompilerParams(vmem_limit_bytes=48 * 2**20),
        cost_estimate=cost(size),
    )(*arrays)


def cost(size):
    return pl.CostEstimate(flops=size * 12, bytes_accessed=size, transcendentals=0)


def place_kernel(*refs, spots, grown):
    k = len(spots)
    src, dst, (buf, in_s, out_s) = refs[:k], refs[k + grown], refs[k + grown + 1 :]
    me = lax.axis_index("dp")
    core, chip = me % 2, me // 2
    cy, cx = chip % 2, chip // 2
    layers, height = src[0].shape[:2]

    def store(z, layer):
        block, other, h = spots[z]
        x = 1 - cx if block in (XN, DG) else cx
        y = 1 - cy if block in (YN, DG) else cy
        owner = 4 * x + 2 * y + (1 - core if other else core)
        rows = pl.ds(pl.multiple_of((2 * owner + h) * height, height), height)
        return pltpu.make_async_copy(buf.at[z, layer], dst.at[layer, rows], out_s.at[z, layer])

    load = lambda z, layer: pltpu.make_async_copy(src[z].at[layer], buf.at[z, layer], in_s.at[z, layer])
    every = [(z, layer) for z in range(k) for layer in range(layers)]
    for one in every:
        load(*one).start()
    for one in every:
        load(*one).wait()
        store(*one).start()
    for one in every:
        store(*one).wait()


def place(pieces, shape, into=None):
    spots, arrays = zip(*pieces)
    grown = into is not None
    size = sum(a.size * 4 for a in arrays)
    return pl.pallas_call(
        functools.partial(place_kernel, spots=spots, grown=int(grown)),
        name="place",
        out_shape=jax.ShapeDtypeStruct(shape, arrays[0].dtype),
        in_specs=[pl.BlockSpec(memory_space=pl.ANY)] * (len(arrays) + grown),
        out_specs=pl.BlockSpec(memory_space=pl.ANY),
        scratch_shapes=[
            pltpu.VMEM((len(arrays), *arrays[0].shape), arrays[0].dtype),
            pltpu.SemaphoreType.DMA((len(arrays), shape[0])),
            pltpu.SemaphoreType.DMA((len(arrays), shape[0])),
        ],
        input_output_aliases={len(arrays): 0} if grown else {},
        compiler_params=pltpu.CompilerParams(vmem_limit_bytes=32 * 2**20),
        cost_estimate=cost(size),
    )(*arrays, *((into,) if grown else ()))


def solution(mesh):
    n = mesh.shape["dp"]

    def step(*arrays):
        terms, weights, m, v = (arrays[i : i + 3] for i in (0, 3, 6, 9))
        layers = weights[0].shape[0]
        blocks = [(one.shape[1] // 2, one.shape[2]) for one in m]
        kinds = (blocks[0], blocks[2])
        count = float(n * sum(one.size for one in m))
        dma = pltpu.SemaphoreType.DMA
        units = 3 * layers
        any_space = pl.BlockSpec(memory_space=pl.ANY)
        out = pl.pallas_call(
            functools.partial(kernel, n=n, layers=layers, count=count),
            name="step",
            out_shape=[jax.ShapeDtypeStruct(one.shape, BF) for one in weights[:KEPT]]
            + [jax.ShapeDtypeStruct((layers, *blocks[KEPT]), BF)] * 2
            + [jax.ShapeDtypeStruct(one.shape, BF) for one in m]
            + [jax.ShapeDtypeStruct((8, 128), F32)],
            in_specs=[any_space] * 12,
            out_specs=[any_space] * (KEPT + 6),
            scratch_shapes=[pltpu.VMEM((4, layers, 2, *b), BF) for b in blocks]
            + [pltpu.VMEM((6, layers, *b), BF) for b in blocks]
            + [pltpu.VMEM((RING, *b), BF) for b in kinds]
            + [pltpu.VMEM((FEED, *b), F32) for b in kinds] * 2
            + [pltpu.VMEM((FEED, *b), BF) for b in kinds]
            + [pltpu.VMEM((n + 1, 8, 128), F32), pltpu.VMEM((8, 128), F32)]
            + [dma((4, units, 2)), dma((4, units, 2)), dma((6, units)), dma((6, units)), dma((2, RING)), dma((3, 2, FEED))]
            + [dma((n,)), dma((n,)), dma((2, units, 2)), dma((2, units, 2)), dma((2, units)), dma((2, units))]
            + [dma((4, units, 2)), dma((4, units, 2)), dma((2, units, 2))],
            compiler_params=pltpu.CompilerParams(collective_id=0, has_side_effects=True, vmem_limit_bytes=62 * 2**20),
        )(*terms, *weights, *m, *v)
        kept, (low, high), sums, factor = out[:KEPT], out[KEPT : KEPT + 2], out[KEPT + 2 : KEPT + 5], out[KEPT + 5][0, 0]

        def hop(a, flip):
            return lax.ppermute(a, "dp", [(i, i ^ flip) for i in range(n)])

        def fresh(i):
            return moments(m[i], v[i], sums[i].astype(F32) * factor)

        x, y, mate = n // 2, n // 4, 1
        x_low, y_high = hop(low, x), hop(high, y)
        m_low, m_high = hop(low, mate), hop(high, mate)
        x_high, y_low = hop(high, x), hop(low, y)
        new = [fresh(0), fresh(1)]
        x_low, y_high, new = lax.optimization_barrier((x_low, y_high, new))
        d_low, d_high = hop(x_low, y), hop(y_high, x)
        mx_low, my_high = hop(x_low, mate), hop(y_high, mate)
        kept = move(*kept)
        new.append(fresh(2))
        x_high, y_low, kept, new = lax.optimization_barrier((x_high, y_low, kept, new))
        mx_high, my_low = hop(x_high, mate), hop(y_low, mate)
        shape = weights[KEPT].shape
        first = [((ME, 0, 0), low), ((ME, 0, 1), high), ((ME, 1, 0), m_low), ((ME, 1, 1), m_high), ((XN, 0, 0), x_low), ((YN, 0, 1), y_high)]
        first += [((XN, 1, 0), mx_low), ((YN, 1, 1), my_high)]
        down = place(first, shape)
        then = [((XN, 0, 1), x_high), ((YN, 0, 0), y_low), ((XN, 1, 1), mx_high), ((YN, 1, 0), my_low)]
        down = place(then, shape, down)
        d_low, d_high, down = lax.optimization_barrier((d_low, d_high, down))
        md_low, md_high = hop(d_low, mate), hop(d_high, mate)
        last = [((DG, 0, 0), d_low), ((DG, 0, 1), d_high), ((DG, 1, 0), md_low), ((DG, 1, 1), md_high)]
        down = place(last, shape, down)
        return (*kept, down, *(one[0] for one in new), *(one[1] for one in new))

    all_of, cut = P(None, None, None), P(None, "dp", None)
    return jax.shard_map(
        step,
        mesh=mesh,
        in_specs=(P(("rep", "dp"), None, None, None),) * 3 + (all_of,) * 3 + (cut,) * 6,
        out_specs=(P("rep", None, None),) * 3 + (P("rep", "dp", None),) * 6,
        check_vma=False,
    )
```

```python
import functools
from typing import NamedTuple

import jax
import jax.numpy as jnp
from jax import lax
from jax.experimental import pallas as pl
from jax.experimental.pallas import tpu as pltpu
from jax.sharding import PartitionSpec as P


BF, F32 = jnp.bfloat16, jnp.float32
RING = 4
FEED = (3, 2)
KEPT = 2
CUT = 4
ME, XN, YN, DG = range(4)
XD, XO, XT, YD, YO, YT = range(6)


def moments(m, v, g):
    return 0.9 * m + 0.1 * g, 0.95 * v + 0.05 * g * g


def neighbours():
    me = lax.axis_index("dp")
    core, chip = me % 2, me // 2
    cy, cx = chip % 2, chip // 2
    owner = lambda block, c: 4 * (1 - cx if block in (XN, DG) else cx) + 2 * (1 - cy if block in (YN, DG) else cy) + c
    return me, core, owner


def kernel(*refs, n, layers, count):
    it = iter(refs)
    take = lambda k: [next(it) for _ in range(k)]
    g, w, m, v = take(3), take(3), take(3), take(3)
    whole, ends, mates, parts, tails, gsum, factor_ref = take(KEPT), take(2), take(2), take(2), take(2), take(3), next(it)
    pair, land = take(3), take(3)
    gring, mring, vring, wring = take(2), take(2), take(2), take(2)
    squares, factor_v = take(2)
    d2d_s, d2d_r, lk_s, lk_r, ring_s, feed_s = take(6)
    sq_s, own_s, fwd_s, rel_s, loc_s, end_s, end_r = take(7)

    me, core, owner = neighbours()
    mate, xnbr, ynbr = owner(ME, 1 - core), owner(XN, core), owner(YN, core)
    across = (xnbr, ynbr)

    def remote(src, dst, s, r, device):
        return pltpu.make_async_remote_copy(
            src_ref=src, dst_ref=dst, send_sem=s, recv_sem=r, device_id={"dp": device}, device_id_type=pl.DeviceIdType.MESH
        )

    barrier = pltpu.get_barrier_semaphore()
    for k in range(1, n):
        pl.semaphore_signal(barrier, inc=1, device_id={"dp": (me + k) % n}, device_id_type=pl.DeviceIdType.MESH)

    units, kind, half = geometry(land, layers)

    def rows(i, device, r0=0, nr=None):
        return pl.ds(pl.multiple_of(device * (2 * half[i]) + r0, 16), 2 * half[i] if nr is None else nr)

    steps = rs_steps(units, half)
    exchanges = exchange_list(steps, half, units)

    def part(step):
        return pair[units[step.u][0]].at[step.block, units[step.u][1], pl.ds(step.h * half[units[step.u][0]] + step.r0, step.nr)]

    def exchange(z):
        block, u, r0, nr = exchanges[z]
        i, layer = units[u]
        src = g[i].at[0, layer, rows(i, owner(block, 1 - core), r0, nr)]
        return remote(src, pair[i].at[block, layer, pl.ds(r0, nr)], d2d_s.at[i], d2d_r.at[z], mate)

    order = {c: [k for k, step in enumerate(steps) if kind[units[step.u][0]] == c] for c in (0, 1)}
    place_of = {k: (c, p) for c in order for p, k in enumerate(order[c])}

    def own_rows(k):
        c, p = place_of[k]
        return gring[c].at[p % RING, pl.ds(0, steps[k].nr)]

    def term(k):
        step = steps[k]
        i, layer = units[step.u]
        c, p = place_of[k]
        src = g[i].at[0, layer, rows(i, owner(step.block, core), step.h * half[i] + step.r0, step.nr)]
        return pltpu.make_async_copy(src, own_rows(k), ring_s.at[c, p % RING])

    def landed(step, stream):
        i, layer = units[step.u]
        return land[i].at[stream, layer, pl.ds(step.r0, step.nr)]

    def push(k):
        step = steps[k]
        return remote(part(step), landed(step, step.stream), lk_s.at[units[step.u][0]], lk_r.at[k], across[step.stream >= YD])

    seen, met = set(), set()

    def arrive(stream, step):
        for k, other in enumerate(steps):
            overlap = other.r0 < step.r0 + step.nr and step.r0 < other.r0 + other.nr
            if other.send and other.stream == stream and other.u == step.u and overlap and k not in seen:
                seen.add(k)
                dst = landed(other, stream)
                remote(dst, dst, lk_s.at[0], lk_r.at[k], xnbr).wait_recv()

    def meet(step):
        first = step.h * half[units[step.u][0]] + step.r0
        for z, (block, u, r0, nr) in enumerate(exchanges):
            if block == step.block and u == step.u and r0 < first + step.nr and first < r0 + nr and z not in met:
                met.add(z)
                i, layer = units[u]
                dst = pair[i].at[block, layer, pl.ds(r0, nr)]
                remote(dst, dst, d2d_s.at[0], d2d_r.at[z], mate).wait_recv()

    fed = make_order(units, half)
    feed_order = {c: [k for k, piece in enumerate(fed) if kind[units[piece[0]][0]] == c] for c in (0, 1)}
    feed_at = {k: p for c in (0, 1) for p, k in enumerate(feed_order[c])}

    def feed_slot(k):
        c = kind[units[fed[k][0]][0]]
        return [ring[c].at[feed_at[k] % FEED[c], pl.ds(0, fed[k][3])] for ring in (mring, vring, wring)]

    def feed(k):
        u, h, r0, nr = fed[k]
        i, layer = units[u]
        c = kind[i]
        slot = feed_at[k] % FEED[c]
        mine = pl.ds(h * half[i] + r0, nr)
        src = (m[i].at[layer, mine], v[i].at[layer, mine], w[i].at[layer, rows(i, me, h * half[i] + r0, nr)])
        return [pltpu.make_async_copy(a, b, feed_s.at[z, c, slot]) for z, (a, b) in enumerate(zip(src, feed_slot(k), strict=True))]

    exchanged, started = 0, {0: 0, 1: 0}

    def next_exchange():
        nonlocal exchanged
        if exchanged < len(exchanges):
            exchange(exchanged).start()
            exchanged += 1

    def next_term(c):
        if started[c] < len(order[c]):
            term(order[c][started[c]]).start()
            started[c] += 1

    next_term(0)
    next_term(0)
    pl.semaphore_wait(barrier, n - 1)
    for _ in range(4):
        next_exchange()
    next_term(0)
    next_term(0)

    def tile_of(cols, nr):
        return min(65536 // cols, nr)

    zero = jnp.zeros((8, 128), F32)
    total = (zero,) * 4
    for k, step in enumerate(steps):
        i, layer = units[step.u]
        c = kind[i]
        dst = part(step)
        meet(step)
        term(k).wait()
        more = []
        for stream in step.needs:
            arrive(stream, step)
            more.append(landed(step, stream))
        own = own_rows(k)
        cols = dst.shape[1]
        tile = tile_of(cols, step.nr)

        def body(r, acc, dst=dst, own=own, more=more, cols=cols, tile=tile, squared=not step.send):
            at_rows = pl.ds(pl.multiple_of(r * tile, tile), tile)
            s = own[at_rows, :].astype(F32) + dst[at_rows, :].astype(F32)
            for one in more:
                s = s + one[at_rows, :].astype(F32)
            b = s.astype(BF)
            dst[at_rows, :] = b
            if squared:
                q = b.astype(F32)
                q = q * q
                acc = list(acc)
                for a in range(tile // 8):
                    for z in range(cols // 128):
                        acc[(a + z) % 4] = acc[(a + z) % 4] + q[8 * a : 8 * a + 8, 128 * z : 128 * z + 128]
                acc = tuple(acc)
            return acc

        if step.send:
            lax.fori_loop(0, step.nr // tile, body, ())
            push(k).start()
        else:
            total = lax.fori_loop(0, step.nr // tile, body, total)
            pltpu.make_async_copy(dst, gsum[i].at[layer, pl.ds(step.h * half[i] + step.r0, step.nr)], loc_s.at[0, i]).start()
        next_term(c)
        next_exchange()
        if k == 5:
            for _ in range(RING):
                next_term(1)
        if k == 20:
            for c in (0, 1):
                for z in feed_order[c][: FEED[c]]:
                    for copy in feed(z):
                        copy.start()

    squares[n] = total[0] + total[1] + total[2] + total[3]
    for k in range(1, n):
        remote(squares.at[n], squares.at[me], sq_s.at[0], sq_s.at[1], (me + k) % n).start()
    for i in range(3):
        remote(pair[i], pair[i], d2d_s.at[i], d2d_r.at[0], mate).wait_send()
        remote(land[i], land[i], lk_s.at[i], lk_r.at[0], xnbr).wait_send()
    squares[me] = squares[n]
    others = squares.at[pl.ds(0, n - 1)]
    remote(others, others, sq_s.at[0], sq_s.at[1], xnbr).wait_recv()
    everything = squares[0]
    for k in range(1, n):
        everything = everything + squares[k]
    everything = jnp.sum(jnp.sum(everything, axis=0, keepdims=True), axis=1, keepdims=True)
    factor = jnp.minimum(1.0, 0.5 * lax.rsqrt(everything / count + 1e-30))
    factor_v[...] = jnp.broadcast_to(factor, (8, 128))

    def out(i, layer, device, r0=0, nr=None):
        return whole[i].at[layer, rows(i, device, r0, nr)]

    gathered = [u for u in range(len(units)) if units[u][0] < KEPT]
    sent = [k for k, piece in enumerate(fed) if piece[0] in gathered]

    for k, (u, h, r0, nr) in enumerate(fed):
        i, layer = units[u]
        c = kind[i]
        for copy in feed(k):
            copy.wait()
        mine = pl.ds(h * half[i] + r0, nr)
        dst, src = pair[i].at[DG, layer, mine], pair[i].at[ME, layer, mine]
        mm, vv, ww = feed_slot(k)
        tile = min(32768 // dst.shape[1] if c else 16, nr)

        def body(r, _, dst=dst, src=src, mm=mm, vv=vv, ww=ww, tile=tile):
            at_rows = pl.ds(pl.multiple_of(r * tile, tile), tile)
            grad = src[at_rows, :].astype(F32) * factor_v[0:1, 0:1]
            m_new, v_new = moments(mm[at_rows, :], vv[at_rows, :], grad)
            weight = ww[at_rows, :].astype(F32)
            dst[at_rows, :] = (weight - 0.02 * (m_new * lax.rsqrt(v_new + 1e-8) + 0.1 * weight)).astype(BF)
            return 0

        lax.fori_loop(0, nr // tile, body, 0)
        if i < KEPT:
            here = out(i, layer, me, h * half[i] + r0, nr)
            z = sent.index(k)
            remote(dst, here, own_s.at[0, i], lk_r.at[z], xnbr).start()
            remote(dst, here, own_s.at[1, i], lk_r.at[len(sent) + z], ynbr).start()
            remote(dst, here, own_s.at[2, i], d2d_r.at[z], mate).start()
            pltpu.make_async_copy(dst, here, loc_s.at[1, i]).start()
        else:
            remote(dst, mates[h].at[layer], end_s.at[0, h], end_r.at[0, h], mate).start()
            pltpu.make_async_copy(dst, ends[h].at[layer], loc_s.at[2, h]).start()
            tail = half[i] // CUT
            pltpu.make_async_copy(dst.at[pl.ds(0, half[i] - tail)], parts[h].at[layer], loc_s.at[3, h]).start()
        if feed_at[k] + FEED[c] < len(feed_order[c]):
            for copy in feed(feed_order[c][feed_at[k] + FEED[c]]):
                copy.start()

    relays = [(u, h, block) for u in gathered for h in range(2) for block in (XN, YN, DG)]

    def relay(u, h, block):
        i, layer = units[u]
        here = out(i, layer, owner(block, core), h * half[i], half[i])
        remote(here, here, rel_s.at[block - 1, i], d2d_r.at[len(sent) + relays.index((u, h, block))], mate).start()

    def forward_sem(u, h):
        return lk_r.at[2 * len(sent) + 2 * u + h]

    def onward(u, h, block, device):
        i, layer = units[u]
        here = out(i, layer, owner(block, core), h * half[i], half[i])
        remote(here, here, fwd_s.at[h, i], forward_sem(u, h), device).start()

    def from_link(u, h, which):
        i, layer = units[u]
        for z, k in enumerate(sent):
            if fed[k][:2] == (u, h):
                there = out(i, layer, owner((XN, YN)[which], core), h * half[i] + fed[k][2], fed[k][3])
                remote(there, there, own_s.at[0, 0], lk_r.at[which * len(sent) + z], xnbr).wait_recv()

    for u in gathered:
        from_link(u, 0, 0)
        onward(u, 0, XN, ynbr)
        relay(u, 0, XN)
        from_link(u, 1, 1)
        onward(u, 1, YN, xnbr)
        relay(u, 1, YN)
        from_link(u, 0, 1)
        relay(u, 0, YN)
        from_link(u, 1, 0)
        relay(u, 1, XN)

    for u, (i, layer) in enumerate(units):
        if i >= KEPT:
            tail = half[i] // CUT
            for h in range(2):
                src = pair[i].at[DG, layer, pl.ds((h + 1) * half[i] - tail, tail)]
                remote(src, tails[h].at[layer], end_s.at[1, h], end_r.at[1, h], across[h]).start()

    for u in gathered:
        i, layer = units[u]
        for h in range(2):
            there = out(i, layer, owner(DG, core), h * half[i], half[i])
            remote(there, there, fwd_s.at[0, 0], forward_sem(u, h), xnbr).wait_recv()
            relay(u, h, DG)

    for i in range(3):
        pltpu.make_async_copy(gsum[i], gsum[i], loc_s.at[0, i]).wait()
    for i in range(KEPT):
        block, part_of = whole[i].at[:, pl.ds(0, 2 * half[i])], whole[i].at[:, pl.ds(0, half[i])]
        pltpu.make_async_copy(block, block, loc_s.at[1, i]).wait()
        for z in range(3):
            remote(block, block, own_s.at[z, i], lk_r.at[0], xnbr).wait_send()
        for h in range(2):
            remote(part_of, part_of, fwd_s.at[h, i], lk_r.at[0], xnbr).wait_send()
    for h in range(2):
        pltpu.make_async_copy(ends[h], ends[h], loc_s.at[2, h]).wait()
        pltpu.make_async_copy(parts[h], parts[h], loc_s.at[3, h]).wait()
        both = remote(mates[h], mates[h], end_s.at[0, h], end_r.at[0, h], mate)
        both.wait_send()
        both.wait_recv()
    remote(others, others, sq_s.at[0], sq_s.at[1], xnbr).wait_send()
    for z, k in enumerate(sent):
        u, h, r0, nr = fed[k]
        i, layer = units[u]
        there = out(i, layer, mate, h * half[i] + r0, nr)
        remote(there, there, own_s.at[0, 0], d2d_r.at[z], mate).wait_recv()
    done = pltpu.make_async_copy(factor_v, factor_ref, loc_s.at[0, 0])
    done.start()
    done.wait()
    for z, (u, h, block) in enumerate(relays):
        i, layer = units[u]
        there = out(i, layer, owner(block, 1 - core), h * half[i], half[i])
        remote(there, there, rel_s.at[0, 0], d2d_r.at[len(sent) + z], mate).wait_recv()
    for i in range(KEPT):
        block = whole[i].at[:, pl.ds(0, 2 * half[i])]
        for z in range(3):
            remote(block, block, rel_s.at[z, i], d2d_r.at[0], mate).wait_send()
    for h in range(2):
        both = remote(tails[h], tails[h], end_s.at[1, h], end_r.at[1, h], xnbr)
        both.wait_send()
        both.wait_recv()


class Step(NamedTuple):
    send: bool
    block: int
    u: int
    h: int
    r0: int
    nr: int
    stream: int | None
    needs: tuple


def geometry(land, layers):
    return [(i, layer) for i in range(3) for layer in range(layers)], (0, 0, 1), [p.shape[2] for p in land]


def cuts(size, shares):
    at = 0
    for share in shares:
        yield at, size * share // 4
        at += size * share // 4


def rs_steps(units, half):
    steps = []
    last = len(units) - 1

    def add(send, u, shares, *two):
        for r0, nr in cuts(half[units[u][0]], shares):
            steps.extend(Step(send, block, u, h, r0, nr, stream, needs) for block, h, stream, needs in two)

    for u in range(last + 1):
        add(True, u, (1, 1, 2) if u == 0 else (4,), (DG, 0, XD, ()), (DG, 1, YD, ()))
    for u in range(last + 1):
        add(True, u, (4,), (XN, 0, XO, ()), (YN, 1, YO, ()))
    for u in range(last + 1):
        add(True, u, (2, 1, 1) if u == last else (4,), (YN, 0, YT, (XD,)), (XN, 1, XT, (YD,)))
    for u in range(last + 1):
        add(False, u, (2, 1, 1) if u == last else (4,), (ME, 0, None, (XO, YT)), (ME, 1, None, (YO, XT)))
    return steps


def exchange_list(steps, half, units):
    first = [(s.block, s.u, s.h * half[units[s.u][0]] + s.r0, s.nr) for s in steps if s.block == DG]
    return first + [(block, u, 0, 2 * half[i]) for two in ((XN, YN), (ME,)) for u, (i, _) in enumerate(units) for block in two]


def make_order(units, half):
    pieces = []
    for u, (i, _) in enumerate(units):
        for r0, nr in cuts(half[i], (1, 3) if u == 0 else (4,)):
            pieces += [(u, 0, r0, nr), (u, 1, r0, nr)]
    return pieces


def cost(size):
    return pl.CostEstimate(flops=size * 12, bytes_accessed=size, transcendentals=0)


def place_kernel(*refs, spots, half, moves, grown):
    k = len(spots)
    pieces_in, whole_in = refs[:k], refs[k : k + moves]
    outs = refs[k + moves + grown :][: moves + 1]
    scratch = refs[k + 2 * moves + grown + 1 :]
    bufs, moved, in_s, out_s = scratch[:k], scratch[k : k + moves], scratch[-2], scratch[-1]
    _, core, owner = neighbours()
    jobs = []
    for a in range(moves):
        layers, height = whole_in[a].shape[:2]
        size = height // 4
        for layer in range(layers):
            for p in range(4):
                at = pl.ds(p * size, size)
                jobs.append((whole_in[a].at[layer, at], moved[a].at[layer, at], outs[a].at[layer, at]))
    for z in range(k):
        block, other, h, r0 = spots[z]
        start = (2 * owner(block, 1 - core if other else core) + h) * half + r0
        at = pl.ds(pl.multiple_of(start, 16), pieces_in[z].shape[1])
        jobs.append((pieces_in[z], bufs[z], outs[moves].at[:, at]))
    loads = [functools.partial(pltpu.make_async_copy, src, buf, in_s.at[j]) for j, (src, buf, _) in enumerate(jobs)]
    stores = [functools.partial(pltpu.make_async_copy, buf, dst, out_s.at[j]) for j, (_, buf, dst) in enumerate(jobs)]
    for load in loads:
        load().start()
    for load, store in zip(loads, stores, strict=True):
        load().wait()
        store().start()
    for store in stores:
        store().wait()


def place(pieces, shape, half, into=None, moves=()):
    spots, arrays = zip(*pieces)
    grown = into is not None
    size = sum(a.size * 4 for a in (*arrays, *moves))
    jobs = len(arrays) + sum(4 * a.shape[0] for a in moves)
    like = [jax.ShapeDtypeStruct(a.shape, a.dtype) for a in moves] + [jax.ShapeDtypeStruct(shape, arrays[0].dtype)]
    in_hbm = pl.BlockSpec(memory_space=pltpu.HBM)
    out = pl.pallas_call(
        functools.partial(place_kernel, spots=spots, half=half, moves=len(moves), grown=int(grown)),
        out_shape=like,
        in_specs=[in_hbm] * (len(arrays) + len(moves) + grown),
        out_specs=[in_hbm] * len(like),
        scratch_shapes=[pltpu.VMEM(a.shape, a.dtype) for a in (*arrays, *moves)] + [pltpu.SemaphoreType.DMA((jobs,))] * 2,
        input_output_aliases={len(arrays) + len(moves): len(moves)} if grown else {},
        compiler_params=pltpu.CompilerParams(vmem_limit_bytes=67043328),
        cost_estimate=cost(size),
    )(*arrays, *moves, *((into,) if grown else ()))
    return out if moves else out[0]


def fresh_kernel(*refs):
    m, v, g, factor_ref, m_new, v_new = refs[:3], refs[3:6], refs[6:9], refs[9], refs[10:13], refs[13:16]
    bufs, in_s, out_s = refs[16:25], refs[25], refs[26]
    pieces = []
    for i in range(3):
        layers, height = m[i].shape[:2]
        pieces += [(i, layer, p * (height // 2), height // 2) for layer in range(layers) for p in range(2)]

    def loads(z):
        i, layer, r0, nr = pieces[z]
        at_rows = pl.ds(r0, nr)
        return [pltpu.make_async_copy(a[i].at[layer, at_rows], bufs[3 * t + i].at[layer, at_rows], in_s.at[t, z]) for t, a in enumerate((m, v, g))]

    def stores(z):
        i, layer, r0, nr = pieces[z]
        at_rows = pl.ds(r0, nr)
        return [pltpu.make_async_copy(bufs[3 * t + i].at[layer, at_rows], a[i].at[layer, at_rows], out_s.at[t, z]) for t, a in enumerate((m_new, v_new))]

    for z in range(len(pieces)):
        for copy in loads(z):
            copy.start()
    for z, (i, layer, r0, nr) in enumerate(pieces):
        for copy in loads(z):
            copy.wait()
        mm, vv, gg = (bufs[3 * t + i].at[layer] for t in range(3))
        tile = 65536 // mm.shape[1]

        def body(r, _, mm=mm, vv=vv, gg=gg, r0=r0, tile=tile):
            at_rows = pl.ds(pl.multiple_of(r0 + r * tile, tile), tile)
            grad = gg[at_rows, :].astype(F32) * factor_ref[0:1, 0:1]
            mm[at_rows, :], vv[at_rows, :] = moments(mm[at_rows, :], vv[at_rows, :], grad)
            return 0

        lax.fori_loop(0, nr // tile, body, 0)
        for copy in stores(z):
            copy.start()
    for z in range(len(pieces)):
        for copy in stores(z):
            copy.wait()


def fresh(m, v, sums, factor):
    pieces = 2 * sum(one.shape[0] for one in m)
    size = sum(one.size * 18 for one in m)
    dma = pltpu.SemaphoreType.DMA
    any_space = pl.BlockSpec(memory_space=pltpu.HBM)
    out = pl.pallas_call(
        fresh_kernel,
        name="fresh",
        out_shape=[jax.ShapeDtypeStruct(one.shape, F32) for one in (*m, *v)],
        in_specs=[any_space] * 9 + [pl.BlockSpec(memory_space=pltpu.VMEM)],
        out_specs=[any_space] * 6,
        scratch_shapes=[pltpu.VMEM(one.shape, one.dtype) for one in (*m, *v, *sums)] + [dma((3, pieces)), dma((2, pieces))],
        compiler_params=pltpu.CompilerParams(vmem_limit_bytes=67043328),
        cost_estimate=cost(size),
    )(*m, *v, *sums, factor)
    return out[:3], out[3:]


def solution(mesh):
    n = mesh.shape["dp"]

    def step(*arrays):
        terms, weights, m, v = (arrays[i : i + 3] for i in (0, 3, 6, 9))
        layers = weights[0].shape[0]
        blocks = [(one.shape[1] // 2, one.shape[2]) for one in m]
        kinds = (blocks[0], blocks[2])
        count = float(n * sum(one.size for one in m))
        dma = pltpu.SemaphoreType.DMA
        units = [(i, layer) for i in range(3) for layer in range(layers)]
        halves = [b[0] for b in blocks]
        steps = rs_steps(units, halves)
        pieces = sum(units[piece[0]][0] < KEPT for piece in make_order(units, halves))
        swaps = max(len(exchange_list(steps, halves, units)), pieces + 6 * KEPT * layers)
        hops = max(sum(one.send for one in steps), 2 * pieces + 2 * KEPT * layers)
        any_space = pl.BlockSpec(memory_space=pl.ANY)
        half, cols = blocks[KEPT]
        tail = half // CUT
        shapes = [one.shape for one in weights[:KEPT]] + [(layers, half, cols)] * 4 + [(layers, half - tail, cols)] * 2 + [(layers, tail, cols)] * 2
        shapes += [one.shape for one in m]
        out = pl.pallas_call(
            functools.partial(kernel, n=n, layers=layers, count=count),
            name="step",
            out_shape=[jax.ShapeDtypeStruct(shape, BF) for shape in shapes] + [jax.ShapeDtypeStruct((8, 128), F32)],
            in_specs=[any_space] * 12,
            out_specs=[any_space] * (len(shapes) + 1),
            scratch_shapes=[pltpu.VMEM((4, layers, 2 * b[0], b[1]), BF) for b in blocks]
            + [pltpu.VMEM((6, layers, *b), BF) for b in blocks]
            + [pltpu.VMEM((RING, *b), BF) for b in kinds]
            + [pltpu.VMEM((size, *b), F32) for size, b in zip(FEED, kinds, strict=True)] * 2
            + [pltpu.VMEM((size, *b), BF) for size, b in zip(FEED, kinds, strict=True)]
            + [pltpu.VMEM((n + 1, 8, 128), F32), pltpu.VMEM((8, 128), F32)]
            + [dma((3,)), dma((swaps,)), dma((3,)), dma((hops,)), dma((2, RING)), dma((3, 2, max(FEED)))]
            + [dma((2,)), dma((3, KEPT)), dma((2, KEPT)), dma((3, KEPT)), dma((4, 3)), dma((2, 2)), dma((2, 2))],
            compiler_params=pltpu.CompilerParams(collective_id=0, has_side_effects=True, vmem_limit_bytes=67043328),
        )(*terms, *weights, *m, *v)
        kept, (low, high), (m_low, m_high), (low_a, high_a), (x_low_b, y_high_b) = (out[i : i + 2] for i in range(0, 10, 2))
        sums, factor = out[10:13], out[13]

        def hop(a, flip):
            return lax.ppermute(a, "dp", [(i, i ^ flip) for i in range(n)])

        barrier = lax.optimization_barrier
        x, y, mate = n // 2, n // 4, 1
        x_low_a, y_high_a = hop(low_a, x), hop(high_a, y)
        x_high, y_low = hop(high, x), hop(low, y)
        mx_b, my_b = hop(x_low_b, mate), hop(y_high_b, mate)
        new_m, new_v = fresh(m, v, sums, factor)
        x_low_a, y_high_a, new_m, new_v = barrier((x_low_a, y_high_a, new_m, new_v))
        d_low_a, d_high_a = hop(x_low_a, y), hop(y_high_a, x)
        d_low_b, d_high_b = hop(x_low_b, y), hop(y_high_b, x)
        mx_a, my_a = hop(x_low_a, mate), hop(y_high_a, mate)
        shape, b = weights[KEPT].shape, half - tail
        first = [((ME, 0, 0, 0), low), ((ME, 0, 1, 0), high), ((ME, 1, 0, 0), m_low), ((ME, 1, 1, 0), m_high)]
        first += [((XN, 0, 0, 0), x_low_a), ((YN, 0, 1, 0), y_high_a), ((XN, 0, 0, b), x_low_b), ((YN, 0, 1, b), y_high_b)]
        first += [((XN, 1, 0, b), mx_b), ((YN, 1, 1, b), my_b)]
        gate, up, down = place(first, shape, half, moves=kept)
        x_high, y_low, gate, up, down = barrier((x_high, y_low, gate, up, down))
        mx_high, my_low = hop(x_high, mate), hop(y_low, mate)
        then = [((XN, 1, 0, 0), mx_a), ((YN, 1, 1, 0), my_a), ((XN, 0, 1, 0), x_high), ((YN, 0, 0, 0), y_low)]
        down = place(then, shape, half, down)
        d_low_a, d_high_a, down = barrier((d_low_a, d_high_a, down))
        md_low_a, md_high_a = hop(d_low_a, mate), hop(d_high_a, mate)
        more = [((XN, 1, 1, 0), mx_high), ((YN, 1, 0, 0), my_low)]
        down = place(more, shape, half, down)
        late_a = [((DG, 0, 0, 0), d_low_a), ((DG, 0, 1, 0), d_high_a), ((DG, 1, 0, 0), md_low_a), ((DG, 1, 1, 0), md_high_a)]
        down = place(late_a, shape, half, down)
        d_low_b, d_high_b, down = barrier((d_low_b, d_high_b, down))
        md_low_b, md_high_b = hop(d_low_b, mate), hop(d_high_b, mate)
        late_b = [((DG, 0, 0, b), d_low_b), ((DG, 0, 1, b), d_high_b), ((DG, 1, 0, b), md_low_b), ((DG, 1, 1, b), md_high_b)]
        down = place(late_b, shape, half, down)
        return (gate, up, down, *new_m, *new_v)

    all_of, cut = P(None, None, None), P(None, "dp", None)
    return jax.shard_map(
        step,
        mesh=mesh,
        in_specs=(P(("rep", "dp"), None, None, None),) * 3 + (all_of,) * 3 + (cut,) * 6,
        out_specs=(P("rep", None, None),) * 3 + (P("rep", "dp", None),) * 6,
        check_vma=False,
    )
```

```python
import functools
from typing import NamedTuple

import jax
import jax.numpy as jnp
from jax import lax
from jax.experimental import pallas as pl
from jax.experimental.pallas import tpu as pltpu
from jax.sharding import PartitionSpec as P


BF, F32 = jnp.bfloat16, jnp.float32
RING = 4
FEED = (3, 2)
KEPT = 2
CUT = 4
ME, XN, YN, DG = range(4)
XD, XO, XT, YD, YO, YT = range(6)


def moments(m, v, g):
    return 0.9 * m + 0.1 * g, 0.95 * v + 0.05 * g * g


def neighbours():
    me = lax.axis_index("dp")
    core, chip = me % 2, me // 2
    cy, cx = chip % 2, chip // 2
    owner = lambda block, c: 4 * (1 - cx if block in (XN, DG) else cx) + 2 * (1 - cy if block in (YN, DG) else cy) + c
    return me, core, owner


def kernel(*refs, n, layers, count):
    it = iter(refs)
    take = lambda k: [next(it) for _ in range(k)]
    g, w, m, v = take(3), take(3), take(3), take(3)
    whole, ends, mates, parts, tails, gsum, factor_ref = take(KEPT), take(2), take(2), take(2), take(2), take(3), next(it)
    pair, land = take(3), take(3)
    gring, mring, vring, wring = take(2), take(2), take(2), take(2)
    squares, factor_v = take(2)
    d2d_s, d2d_r, lk_s, lk_r, ring_s, feed_s = take(6)
    sq_s, own_s, fwd_s, rel_s, loc_s, end_s, end_r = take(7)

    me, core, owner = neighbours()
    mate, xnbr, ynbr = owner(ME, 1 - core), owner(XN, core), owner(YN, core)
    across = (xnbr, ynbr)

    def remote(src, dst, s, r, device):
        return pltpu.make_async_remote_copy(
            src_ref=src, dst_ref=dst, send_sem=s, recv_sem=r, device_id={"dp": device}, device_id_type=pl.DeviceIdType.MESH
        )

    barrier = pltpu.get_barrier_semaphore()
    for k in range(1, n):
        pl.semaphore_signal(barrier, inc=1, device_id={"dp": (me + k) % n}, device_id_type=pl.DeviceIdType.MESH)

    units, kind, half = geometry(land, layers)

    def rows(i, device, r0=0, nr=None):
        return pl.ds(pl.multiple_of(device * (2 * half[i]) + r0, 16), 2 * half[i] if nr is None else nr)

    steps = rs_steps(units, half)
    exchanges = exchange_list(steps, half, units)

    def part(step):
        return pair[units[step.u][0]].at[step.block, units[step.u][1], pl.ds(step.h * half[units[step.u][0]] + step.r0, step.nr)]

    def exchange(z):
        block, u, r0, nr = exchanges[z]
        i, layer = units[u]
        src = g[i].at[0, layer, rows(i, owner(block, 1 - core), r0, nr)]
        return remote(src, pair[i].at[block, layer, pl.ds(r0, nr)], d2d_s.at[i], d2d_r.at[z], mate)

    order = {c: [k for k, step in enumerate(steps) if kind[units[step.u][0]] == c] for c in (0, 1)}
    place_of = {k: (c, p) for c in order for p, k in enumerate(order[c])}

    def own_rows(k):
        c, p = place_of[k]
        return gring[c].at[p % RING, pl.ds(0, steps[k].nr)]

    def term(k):
        step = steps[k]
        i, layer = units[step.u]
        c, p = place_of[k]
        src = g[i].at[0, layer, rows(i, owner(step.block, core), step.h * half[i] + step.r0, step.nr)]
        return pltpu.make_async_copy(src, own_rows(k), ring_s.at[c, p % RING])

    def landed(step, stream):
        i, layer = units[step.u]
        return land[i].at[stream, layer, pl.ds(step.r0, step.nr)]

    def push(k):
        step = steps[k]
        return remote(part(step), landed(step, step.stream), lk_s.at[units[step.u][0]], lk_r.at[k], across[step.stream >= YD])

    seen, met = set(), set()

    def arrive(stream, step):
        for k, other in enumerate(steps):
            overlap = other.r0 < step.r0 + step.nr and step.r0 < other.r0 + other.nr
            if other.send and other.stream == stream and other.u == step.u and overlap and k not in seen:
                seen.add(k)
                dst = landed(other, stream)
                remote(dst, dst, lk_s.at[0], lk_r.at[k], xnbr).wait_recv()

    def meet(step):
        first = step.h * half[units[step.u][0]] + step.r0
        for z, (block, u, r0, nr) in enumerate(exchanges):
            if block == step.block and u == step.u and r0 < first + step.nr and first < r0 + nr and z not in met:
                met.add(z)
                i, layer = units[u]
                dst = pair[i].at[block, layer, pl.ds(r0, nr)]
                remote(dst, dst, d2d_s.at[0], d2d_r.at[z], mate).wait_recv()

    fed = make_order(units, half)
    feed_order = {c: [k for k, piece in enumerate(fed) if kind[units[piece[0]][0]] == c] for c in (0, 1)}
    feed_at = {k: p for c in (0, 1) for p, k in enumerate(feed_order[c])}

    def feed_slot(k):
        c = kind[units[fed[k][0]][0]]
        return [ring[c].at[feed_at[k] % FEED[c], pl.ds(0, fed[k][3])] for ring in (mring, vring, wring)]

    def feed(k):
        u, h, r0, nr = fed[k]
        i, layer = units[u]
        c = kind[i]
        slot = feed_at[k] % FEED[c]
        mine = pl.ds(h * half[i] + r0, nr)
        src = (m[i].at[layer, mine], v[i].at[layer, mine], w[i].at[layer, rows(i, me, h * half[i] + r0, nr)])
        return [pltpu.make_async_copy(a, b, feed_s.at[z, c, slot]) for z, (a, b) in enumerate(zip(src, feed_slot(k), strict=True))]

    exchanged, started = 0, {0: 0, 1: 0}

    def next_exchange():
        nonlocal exchanged
        if exchanged < len(exchanges):
            exchange(exchanged).start()
            exchanged += 1

    def next_term(c):
        if started[c] < len(order[c]):
            term(order[c][started[c]]).start()
            started[c] += 1

    next_term(0)
    next_term(0)
    pl.semaphore_wait(barrier, n - 1)
    for _ in range(4):
        next_exchange()
    next_term(0)
    next_term(0)

    def tile_of(cols, nr):
        return min(65536 // cols, nr)

    zero = jnp.zeros((8, 128), F32)
    total = (zero,) * 4
    for k, step in enumerate(steps):
        i, layer = units[step.u]
        c = kind[i]
        dst = part(step)
        meet(step)
        term(k).wait()
        more = []
        for stream in step.needs:
            arrive(stream, step)
            more.append(landed(step, stream))
        own = own_rows(k)
        cols = dst.shape[1]
        tile = tile_of(cols, step.nr)

        def body(r, acc, dst=dst, own=own, more=more, cols=cols, tile=tile, squared=not step.send):
            at_rows = pl.ds(pl.multiple_of(r * tile, tile), tile)
            s = own[at_rows, :].astype(F32) + dst[at_rows, :].astype(F32)
            for one in more:
                s = s + one[at_rows, :].astype(F32)
            b = s.astype(BF)
            dst[at_rows, :] = b
            if squared:
                q = b.astype(F32)
                q = q * q
                acc = list(acc)
                for a in range(tile // 8):
                    for z in range(cols // 128):
                        acc[(a + z) % 4] = acc[(a + z) % 4] + q[8 * a : 8 * a + 8, 128 * z : 128 * z + 128]
                acc = tuple(acc)
            return acc

        if step.send:
            lax.fori_loop(0, step.nr // tile, body, ())
            push(k).start()
        else:
            total = lax.fori_loop(0, step.nr // tile, body, total)
            pltpu.make_async_copy(dst, gsum[i].at[layer, pl.ds(step.h * half[i] + step.r0, step.nr)], loc_s.at[0, i]).start()
        next_term(c)
        next_exchange()
        if k == 5:
            for _ in range(RING):
                next_term(1)
        if k == 20:
            for c in (0, 1):
                for z in feed_order[c][: FEED[c]]:
                    for copy in feed(z):
                        copy.start()

    squares[n] = total[0] + total[1] + total[2] + total[3]
    for k in range(1, n):
        remote(squares.at[n], squares.at[me], sq_s.at[0], sq_s.at[1], (me + k) % n).start()
    for i in range(3):
        remote(pair[i], pair[i], d2d_s.at[i], d2d_r.at[0], mate).wait_send()
        remote(land[i], land[i], lk_s.at[i], lk_r.at[0], xnbr).wait_send()
    squares[me] = squares[n]
    others = squares.at[pl.ds(0, n - 1)]
    remote(others, others, sq_s.at[0], sq_s.at[1], xnbr).wait_recv()
    everything = squares[0]
    for k in range(1, n):
        everything = everything + squares[k]
    everything = jnp.sum(jnp.sum(everything, axis=0, keepdims=True), axis=1, keepdims=True)
    factor = jnp.minimum(1.0, 0.5 * lax.rsqrt(everything / count + 1e-30))
    factor_v[...] = jnp.broadcast_to(factor, (8, 128))

    def out(i, layer, device, r0=0, nr=None):
        return whole[i].at[layer, rows(i, device, r0, nr)]

    gathered = [u for u in range(len(units)) if units[u][0] < KEPT]
    sent = [k for k, piece in enumerate(fed) if piece[0] in gathered]

    for k, (u, h, r0, nr) in enumerate(fed):
        i, layer = units[u]
        c = kind[i]
        for copy in feed(k):
            copy.wait()
        mine = pl.ds(h * half[i] + r0, nr)
        dst, src = pair[i].at[DG, layer, mine], pair[i].at[ME, layer, mine]
        mm, vv, ww = feed_slot(k)
        tile = min(32768 // dst.shape[1] if c else 16, nr)

        def body(r, _, dst=dst, src=src, mm=mm, vv=vv, ww=ww, tile=tile):
            at_rows = pl.ds(pl.multiple_of(r * tile, tile), tile)
            grad = src[at_rows, :].astype(F32) * factor_v[0:1, 0:1]
            m_new, v_new = moments(mm[at_rows, :], vv[at_rows, :], grad)
            weight = ww[at_rows, :].astype(F32)
            dst[at_rows, :] = (weight - 0.02 * (m_new * lax.rsqrt(v_new + 1e-8) + 0.1 * weight)).astype(BF)
            return 0

        lax.fori_loop(0, nr // tile, body, 0)
        if i < KEPT:
            here = out(i, layer, me, h * half[i] + r0, nr)
            z = sent.index(k)
            remote(dst, here, own_s.at[0, i], lk_r.at[z], xnbr).start()
            remote(dst, here, own_s.at[1, i], lk_r.at[len(sent) + z], ynbr).start()
            remote(dst, here, own_s.at[2, i], d2d_r.at[z], mate).start()
            pltpu.make_async_copy(dst, here, loc_s.at[1, i]).start()
        else:
            remote(dst, mates[h].at[layer], end_s.at[0, h], end_r.at[0, h], mate).start()
            pltpu.make_async_copy(dst, ends[h].at[layer], loc_s.at[2, h]).start()
            tail = half[i] // CUT
            pltpu.make_async_copy(dst.at[pl.ds(0, half[i] - tail)], parts[h].at[layer], loc_s.at[3, h]).start()
        if feed_at[k] + FEED[c] < len(feed_order[c]):
            for copy in feed(feed_order[c][feed_at[k] + FEED[c]]):
                copy.start()

    relays = [(u, h, block) for u in gathered for h in range(2) for block in (XN, YN, DG)]

    def relay(u, h, block):
        i, layer = units[u]
        here = out(i, layer, owner(block, core), h * half[i], half[i])
        remote(here, here, rel_s.at[block - 1, i], d2d_r.at[len(sent) + relays.index((u, h, block))], mate).start()

    def forward_sem(u, h):
        return lk_r.at[2 * len(sent) + 2 * u + h]

    def onward(u, h, block, device):
        i, layer = units[u]
        here = out(i, layer, owner(block, core), h * half[i], half[i])
        remote(here, here, fwd_s.at[h, i], forward_sem(u, h), device).start()

    def from_link(u, h, which):
        i, layer = units[u]
        for z, k in enumerate(sent):
            if fed[k][:2] == (u, h):
                there = out(i, layer, owner((XN, YN)[which], core), h * half[i] + fed[k][2], fed[k][3])
                remote(there, there, own_s.at[0, 0], lk_r.at[which * len(sent) + z], xnbr).wait_recv()

    for u in gathered:
        from_link(u, 0, 0)
        onward(u, 0, XN, ynbr)
        relay(u, 0, XN)
        from_link(u, 1, 1)
        onward(u, 1, YN, xnbr)
        relay(u, 1, YN)
        from_link(u, 0, 1)
        relay(u, 0, YN)
        from_link(u, 1, 0)
        relay(u, 1, XN)

    for u, (i, layer) in enumerate(units):
        if i >= KEPT:
            tail = half[i] // CUT
            for h in range(2):
                src = pair[i].at[DG, layer, pl.ds((h + 1) * half[i] - tail, tail)]
                remote(src, tails[h].at[layer], end_s.at[1, h], end_r.at[1, h], across[h]).start()

    for u in gathered:
        i, layer = units[u]
        for h in range(2):
            there = out(i, layer, owner(DG, core), h * half[i], half[i])
            remote(there, there, fwd_s.at[0, 0], forward_sem(u, h), xnbr).wait_recv()
            relay(u, h, DG)

    for i in range(3):
        pltpu.make_async_copy(gsum[i], gsum[i], loc_s.at[0, i]).wait()
    for i in range(KEPT):
        block, part_of = whole[i].at[:, pl.ds(0, 2 * half[i])], whole[i].at[:, pl.ds(0, half[i])]
        pltpu.make_async_copy(block, block, loc_s.at[1, i]).wait()
        for z in range(3):
            remote(block, block, own_s.at[z, i], lk_r.at[0], xnbr).wait_send()
        for h in range(2):
            remote(part_of, part_of, fwd_s.at[h, i], lk_r.at[0], xnbr).wait_send()
    for h in range(2):
        pltpu.make_async_copy(ends[h], ends[h], loc_s.at[2, h]).wait()
        pltpu.make_async_copy(parts[h], parts[h], loc_s.at[3, h]).wait()
        both = remote(mates[h], mates[h], end_s.at[0, h], end_r.at[0, h], mate)
        both.wait_send()
        both.wait_recv()
    remote(others, others, sq_s.at[0], sq_s.at[1], xnbr).wait_send()
    for z, k in enumerate(sent):
        u, h, r0, nr = fed[k]
        i, layer = units[u]
        there = out(i, layer, mate, h * half[i] + r0, nr)
        remote(there, there, own_s.at[0, 0], d2d_r.at[z], mate).wait_recv()
    done = pltpu.make_async_copy(factor_v, factor_ref, loc_s.at[0, 0])
    done.start()
    done.wait()
    for z, (u, h, block) in enumerate(relays):
        i, layer = units[u]
        there = out(i, layer, owner(block, 1 - core), h * half[i], half[i])
        remote(there, there, rel_s.at[0, 0], d2d_r.at[len(sent) + z], mate).wait_recv()
    for i in range(KEPT):
        block = whole[i].at[:, pl.ds(0, 2 * half[i])]
        for z in range(3):
            remote(block, block, rel_s.at[z, i], d2d_r.at[0], mate).wait_send()
    for h in range(2):
        both = remote(tails[h], tails[h], end_s.at[1, h], end_r.at[1, h], xnbr)
        both.wait_send()
        both.wait_recv()


class Step(NamedTuple):
    send: bool
    block: int
    u: int
    h: int
    r0: int
    nr: int
    stream: int | None
    needs: tuple


def geometry(land, layers):
    return [(i, layer) for i in range(3) for layer in range(layers)], (0, 0, 1), [p.shape[2] for p in land]


def cuts(size, shares):
    at = 0
    for share in shares:
        yield at, size * share // 4
        at += size * share // 4


def rs_steps(units, half):
    steps = []
    last = len(units) - 1

    def add(send, u, shares, *two):
        for r0, nr in cuts(half[units[u][0]], shares):
            steps.extend(Step(send, block, u, h, r0, nr, stream, needs) for block, h, stream, needs in two)

    for u in range(last + 1):
        add(True, u, (1, 1, 2) if u == 0 else (4,), (DG, 0, XD, ()), (DG, 1, YD, ()))
    for u in range(last + 1):
        add(True, u, (4,), (XN, 0, XO, ()), (YN, 1, YO, ()))
    for u in range(last + 1):
        add(True, u, (2, 1, 1) if u == last else (4,), (YN, 0, YT, (XD,)), (XN, 1, XT, (YD,)))
    for u in range(last + 1):
        add(False, u, (2, 1, 1) if u == last else (4,), (ME, 0, None, (XO, YT)), (ME, 1, None, (YO, XT)))
    return steps


def exchange_list(steps, half, units):
    first = [(s.block, s.u, s.h * half[units[s.u][0]] + s.r0, s.nr) for s in steps if s.block == DG]
    return first + [(block, u, 0, 2 * half[i]) for two in ((XN, YN), (ME,)) for u, (i, _) in enumerate(units) for block in two]


def make_order(units, half):
    pieces = []
    for u, (i, _) in enumerate(units):
        for r0, nr in cuts(half[i], (1, 3) if u == 0 else (4,)):
            pieces += [(u, 0, r0, nr), (u, 1, r0, nr)]
    return pieces


def cost(size):
    return pl.CostEstimate(flops=size * 12, bytes_accessed=size, transcendentals=0)


def place_kernel(*refs, spots, half, moves, grown):
    k = len(spots)
    pieces_in, whole_in = refs[:k], refs[k : k + moves]
    outs = refs[k + moves + grown :][: moves + 1]
    scratch = refs[k + 2 * moves + grown + 1 :]
    bufs, moved, in_s, out_s = scratch[:k], scratch[k : k + moves], scratch[-2], scratch[-1]
    _, core, owner = neighbours()
    jobs = []
    for a in range(moves):
        layers, height = whole_in[a].shape[:2]
        size = height // 4
        for layer in range(layers):
            for p in range(4):
                at = pl.ds(p * size, size)
                jobs.append((whole_in[a].at[layer, at], moved[a].at[layer, at], outs[a].at[layer, at]))
    for z in range(k):
        block, other, h, r0 = spots[z]
        start = (2 * owner(block, 1 - core if other else core) + h) * half + r0
        at = pl.ds(pl.multiple_of(start, 16), pieces_in[z].shape[1])
        jobs.append((pieces_in[z], bufs[z], outs[moves].at[:, at]))
    loads = [functools.partial(pltpu.make_async_copy, src, buf, in_s.at[j]) for j, (src, buf, _) in enumerate(jobs)]
    stores = [functools.partial(pltpu.make_async_copy, buf, dst, out_s.at[j]) for j, (_, buf, dst) in enumerate(jobs)]
    for load in loads:
        load().start()
    for load, store in zip(loads, stores, strict=True):
        load().wait()
        store().start()
    for store in stores:
        store().wait()


def place(pieces, shape, half, into=None, moves=()):
    spots, arrays = zip(*pieces)
    grown = into is not None
    size = sum(a.size * 4 for a in (*arrays, *moves))
    jobs = len(arrays) + sum(4 * a.shape[0] for a in moves)
    like = [jax.ShapeDtypeStruct(a.shape, a.dtype) for a in moves] + [jax.ShapeDtypeStruct(shape, arrays[0].dtype)]
    in_hbm = pl.BlockSpec(memory_space=pltpu.HBM)
    out = pl.pallas_call(
        functools.partial(place_kernel, spots=spots, half=half, moves=len(moves), grown=int(grown)),
        out_shape=like,
        in_specs=[in_hbm] * (len(arrays) + len(moves) + grown),
        out_specs=[in_hbm] * len(like),
        scratch_shapes=[pltpu.VMEM(a.shape, a.dtype) for a in (*arrays, *moves)] + [pltpu.SemaphoreType.DMA((jobs,))] * 2,
        input_output_aliases={len(arrays) + len(moves): len(moves)} if grown else {},
        compiler_params=pltpu.CompilerParams(vmem_limit_bytes=67043328),
        cost_estimate=cost(size),
    )(*arrays, *moves, *((into,) if grown else ()))
    return out if moves else out[0]


def fresh_kernel(*refs):
    m, v, g, factor_ref, m_new, v_new = refs[:3], refs[3:6], refs[6:9], refs[9], refs[10:13], refs[13:16]
    bufs, in_s, out_s = refs[16:25], refs[25], refs[26]
    pieces = []
    for i in range(3):
        layers, height = m[i].shape[:2]
        pieces += [(i, layer, p * (height // 2), height // 2) for layer in range(layers) for p in range(2)]

    def loads(z):
        i, layer, r0, nr = pieces[z]
        at_rows = pl.ds(r0, nr)
        return [pltpu.make_async_copy(a[i].at[layer, at_rows], bufs[3 * t + i].at[layer, at_rows], in_s.at[t, z]) for t, a in enumerate((m, v, g))]

    def stores(z):
        i, layer, r0, nr = pieces[z]
        at_rows = pl.ds(r0, nr)
        return [pltpu.make_async_copy(bufs[3 * t + i].at[layer, at_rows], a[i].at[layer, at_rows], out_s.at[t, z]) for t, a in enumerate((m_new, v_new))]

    for z in range(len(pieces)):
        for copy in loads(z):
            copy.start()
    for z, (i, layer, r0, nr) in enumerate(pieces):
        for copy in loads(z):
            copy.wait()
        mm, vv, gg = (bufs[3 * t + i].at[layer] for t in range(3))
        tile = 65536 // mm.shape[1]

        def body(r, _, mm=mm, vv=vv, gg=gg, r0=r0, tile=tile):
            at_rows = pl.ds(pl.multiple_of(r0 + r * tile, tile), tile)
            grad = gg[at_rows, :].astype(F32) * factor_ref[0:1, 0:1]
            mm[at_rows, :], vv[at_rows, :] = moments(mm[at_rows, :], vv[at_rows, :], grad)
            return 0

        lax.fori_loop(0, nr // tile, body, 0)
        for copy in stores(z):
            copy.start()
    for z in range(len(pieces)):
        for copy in stores(z):
            copy.wait()


def fresh(m, v, sums, factor):
    pieces = 2 * sum(one.shape[0] for one in m)
    size = sum(one.size * 18 for one in m)
    dma = pltpu.SemaphoreType.DMA
    any_space = pl.BlockSpec(memory_space=pltpu.HBM)
    out = pl.pallas_call(
        fresh_kernel,
        name="fresh",
        out_shape=[jax.ShapeDtypeStruct(one.shape, F32) for one in (*m, *v)],
        in_specs=[any_space] * 9 + [pl.BlockSpec(memory_space=pltpu.VMEM)],
        out_specs=[any_space] * 6,
        scratch_shapes=[pltpu.VMEM(one.shape, one.dtype) for one in (*m, *v, *sums)] + [dma((3, pieces)), dma((2, pieces))],
        compiler_params=pltpu.CompilerParams(vmem_limit_bytes=67043328),
        cost_estimate=cost(size),
    )(*m, *v, *sums, factor)
    return out[:3], out[3:]


def solution(mesh):
    n = mesh.shape["dp"]

    def step(*arrays):
        terms, weights, m, v = (arrays[i : i + 3] for i in (0, 3, 6, 9))
        layers = weights[0].shape[0]
        blocks = [(one.shape[1] // 2, one.shape[2]) for one in m]
        kinds = (blocks[0], blocks[2])
        count = float(n * sum(one.size for one in m))
        dma = pltpu.SemaphoreType.DMA
        units = [(i, layer) for i in range(3) for layer in range(layers)]
        halves = [b[0] for b in blocks]
        steps = rs_steps(units, halves)
        pieces = sum(units[piece[0]][0] < KEPT for piece in make_order(units, halves))
        swaps = max(len(exchange_list(steps, halves, units)), pieces + 6 * KEPT * layers)
        hops = max(sum(one.send for one in steps), 2 * pieces + 2 * KEPT * layers)
        any_space = pl.BlockSpec(memory_space=pl.ANY)
        half, cols = blocks[KEPT]
        tail = half // CUT
        shapes = [one.shape for one in weights[:KEPT]] + [(layers, half, cols)] * 4 + [(layers, half - tail, cols)] * 2 + [(layers, tail, cols)] * 2
        shapes += [one.shape for one in m]
        out = pl.pallas_call(
            functools.partial(kernel, n=n, layers=layers, count=count),
            name="step",
            out_shape=[jax.ShapeDtypeStruct(shape, BF) for shape in shapes] + [jax.ShapeDtypeStruct((8, 128), F32)],
            in_specs=[any_space] * 12,
            out_specs=[any_space] * (len(shapes) + 1),
            scratch_shapes=[pltpu.VMEM((4, layers, 2 * b[0], b[1]), BF) for b in blocks]
            + [pltpu.VMEM((6, layers, *b), BF) for b in blocks]
            + [pltpu.VMEM((RING, *b), BF) for b in kinds]
            + [pltpu.VMEM((size, *b), F32) for size, b in zip(FEED, kinds, strict=True)] * 2
            + [pltpu.VMEM((size, *b), BF) for size, b in zip(FEED, kinds, strict=True)]
            + [pltpu.VMEM((n + 1, 8, 128), F32), pltpu.VMEM((8, 128), F32)]
            + [dma((3,)), dma((swaps,)), dma((3,)), dma((hops,)), dma((2, RING)), dma((3, 2, max(FEED)))]
            + [dma((2,)), dma((3, KEPT)), dma((2, KEPT)), dma((3, KEPT)), dma((4, 3)), dma((2, 2)), dma((2, 2))],
            compiler_params=pltpu.CompilerParams(collective_id=0, has_side_effects=True, vmem_limit_bytes=67043328),
        )(*terms, *weights, *m, *v)
        kept, (low, high), (m_low, m_high), (low_a, high_a), (x_low_b, y_high_b) = (out[i : i + 2] for i in range(0, 10, 2))
        sums, factor = out[10:13], out[13]

        def hop(a, flip):
            return lax.ppermute(a, "dp", [(i, i ^ flip) for i in range(n)])

        barrier = lax.optimization_barrier
        x, y, mate = n // 2, n // 4, 1
        x_low_a, y_high_a = hop(low_a, x), hop(high_a, y)
        x_high, y_low = hop(high, x), hop(low, y)
        mx_b, my_b = hop(x_low_b, mate), hop(y_high_b, mate)
        new_m, new_v = fresh(m, v, sums, factor)
        x_low_a, y_high_a, new_m, new_v = barrier((x_low_a, y_high_a, new_m, new_v))
        d_low_a, d_high_a = hop(x_low_a, y), hop(y_high_a, x)
        d_low_b, d_high_b = hop(x_low_b, y), hop(y_high_b, x)
        mx_a, my_a = hop(x_low_a, mate), hop(y_high_a, mate)
        shape, b = weights[KEPT].shape, half - tail
        first = [((ME, 0, 0, 0), low), ((ME, 0, 1, 0), high), ((ME, 1, 0, 0), m_low), ((ME, 1, 1, 0), m_high)]
        first += [((XN, 0, 0, 0), x_low_a), ((YN, 0, 1, 0), y_high_a), ((XN, 0, 0, b), x_low_b), ((YN, 0, 1, b), y_high_b)]
        first += [((XN, 1, 0, b), mx_b), ((YN, 1, 1, b), my_b)]
        gate, up, down = place(first, shape, half, moves=kept)
        x_high, y_low, gate, up, down = barrier((x_high, y_low, gate, up, down))
        mx_high, my_low = hop(x_high, mate), hop(y_low, mate)
        then = [((XN, 1, 0, 0), mx_a), ((YN, 1, 1, 0), my_a), ((XN, 0, 1, 0), x_high), ((YN, 0, 0, 0), y_low)]
        down = place(then, shape, half, down)
        d_low_a, d_high_a, down = barrier((d_low_a, d_high_a, down))
        md_low_a, md_high_a = hop(d_low_a, mate), hop(d_high_a, mate)
        more = [((XN, 1, 1, 0), mx_high), ((YN, 1, 0, 0), my_low), ((DG, 0, 0, 0), d_low_a), ((DG, 0, 1, 0), d_high_a)]
        down = place(more, shape, half, down)
        d_low_b, d_high_b, down = barrier((d_low_b, d_high_b, down))
        md_low_b, md_high_b = hop(d_low_b, mate), hop(d_high_b, mate)
        down = place([((DG, 1, 0, 0), md_low_a), ((DG, 1, 1, 0), md_high_a)], shape, half, down)
        late_b = [((DG, 0, 0, b), d_low_b), ((DG, 0, 1, b), d_high_b), ((DG, 1, 0, b), md_low_b), ((DG, 1, 1, b), md_high_b)]
        down = place(late_b, shape, half, down)
        return (gate, up, down, *new_m, *new_v)

    all_of, cut = P(None, None, None), P(None, "dp", None)
    return jax.shard_map(
        step,
        mesh=mesh,
        in_specs=(P(("rep", "dp"), None, None, None),) * 3 + (all_of,) * 3 + (cut,) * 6,
        out_specs=(P("rep", None, None),) * 3 + (P("rep", "dp", None),) * 6,
        check_vma=False,
    )
```

```python
import functools
from typing import NamedTuple

import jax
import jax.numpy as jnp
from jax import lax
from jax.experimental import pallas as pl
from jax.experimental.pallas import tpu as pltpu
from jax.sharding import PartitionSpec as P


BF, F32 = jnp.bfloat16, jnp.float32
RING = 4
FEED = (3, 2)
KEPT = 2
CUT = 4
ME, XN, YN, DG = range(4)
XD, XO, XT, YD, YO, YT = range(6)


def moments(m, v, g):
    return 0.9 * m + 0.1 * g, 0.95 * v + 0.05 * g * g


def neighbours():
    me = lax.axis_index("dp")
    core, chip = me % 2, me // 2
    cy, cx = chip % 2, chip // 2
    owner = lambda block, c: 4 * (1 - cx if block in (XN, DG) else cx) + 2 * (1 - cy if block in (YN, DG) else cy) + c
    return me, core, owner


def kernel(*refs, n, layers, count):
    it = iter(refs)
    take = lambda k: [next(it) for _ in range(k)]
    g, w, m, v = take(3), take(3), take(3), take(3)
    whole, ends, mates, parts, tails, gsum, factor_ref = take(KEPT), take(2), take(2), take(2), take(2), take(3), next(it)
    pair, land = take(3), take(3)
    gring, mring, vring, wring = take(2), take(2), take(2), take(2)
    squares, factor_v = take(2)
    d2d_s, d2d_r, lk_s, lk_r, ring_s, feed_s = take(6)
    sq_s, own_s, fwd_s, rel_s, loc_s, end_s, end_r = take(7)

    me, core, owner = neighbours()
    mate, xnbr, ynbr = owner(ME, 1 - core), owner(XN, core), owner(YN, core)
    across = (xnbr, ynbr)

    def remote(src, dst, s, r, device):
        return pltpu.make_async_remote_copy(
            src_ref=src, dst_ref=dst, send_sem=s, recv_sem=r, device_id={"dp": device}, device_id_type=pl.DeviceIdType.MESH
        )

    barrier = pltpu.get_barrier_semaphore()
    for device in (mate, xnbr, ynbr):
        pl.semaphore_signal(barrier, inc=1, device_id={"dp": device}, device_id_type=pl.DeviceIdType.MESH)

    units, kind, half = geometry(land, layers)

    def rows(i, device, r0=0, nr=None):
        return pl.ds(pl.multiple_of(device * (2 * half[i]) + r0, 16), 2 * half[i] if nr is None else nr)

    steps = rs_steps(units, half)
    exchanges = exchange_list(steps, half, units)

    def part(step):
        return pair[units[step.u][0]].at[step.block, units[step.u][1], pl.ds(step.h * half[units[step.u][0]] + step.r0, step.nr)]

    def exchange(z):
        block, u, r0, nr = exchanges[z]
        i, layer = units[u]
        src = g[i].at[0, layer, rows(i, owner(block, 1 - core), r0, nr)]
        return remote(src, pair[i].at[block, layer, pl.ds(r0, nr)], d2d_s.at[i], d2d_r.at[z], mate)

    order = {c: [k for k, step in enumerate(steps) if kind[units[step.u][0]] == c] for c in (0, 1)}
    place_of = {k: (c, p) for c in order for p, k in enumerate(order[c])}

    def own_rows(k):
        c, p = place_of[k]
        return gring[c].at[p % RING, pl.ds(0, steps[k].nr)]

    def term(k):
        step = steps[k]
        i, layer = units[step.u]
        c, p = place_of[k]
        src = g[i].at[0, layer, rows(i, owner(step.block, core), step.h * half[i] + step.r0, step.nr)]
        return pltpu.make_async_copy(src, own_rows(k), ring_s.at[c, p % RING])

    def landed(step, stream):
        i, layer = units[step.u]
        return land[i].at[stream, layer, pl.ds(step.r0, step.nr)]

    def push(k):
        step = steps[k]
        return remote(part(step), landed(step, step.stream), lk_s.at[units[step.u][0]], lk_r.at[k], across[step.stream >= YD])

    seen, met = set(), set()

    def arrive(stream, step):
        for k, other in enumerate(steps):
            overlap = other.r0 < step.r0 + step.nr and step.r0 < other.r0 + other.nr
            if other.send and other.stream == stream and other.u == step.u and overlap and k not in seen:
                seen.add(k)
                dst = landed(other, stream)
                remote(dst, dst, lk_s.at[0], lk_r.at[k], xnbr).wait_recv()

    def meet(step):
        first = step.h * half[units[step.u][0]] + step.r0
        for z, (block, u, r0, nr) in enumerate(exchanges):
            if block == step.block and u == step.u and r0 < first + step.nr and first < r0 + nr and z not in met:
                met.add(z)
                i, layer = units[u]
                dst = pair[i].at[block, layer, pl.ds(r0, nr)]
                remote(dst, dst, d2d_s.at[0], d2d_r.at[z], mate).wait_recv()

    fed = make_order(units, half)
    feed_order = {c: [k for k, piece in enumerate(fed) if kind[units[piece[0]][0]] == c] for c in (0, 1)}
    feed_at = {k: p for c in (0, 1) for p, k in enumerate(feed_order[c])}

    def feed_slot(k):
        c = kind[units[fed[k][0]][0]]
        return [ring[c].at[feed_at[k] % FEED[c], pl.ds(0, fed[k][3])] for ring in (mring, vring, wring)]

    def feed(k):
        u, h, r0, nr = fed[k]
        i, layer = units[u]
        c = kind[i]
        slot = feed_at[k] % FEED[c]
        mine = pl.ds(h * half[i] + r0, nr)
        src = (m[i].at[layer, mine], v[i].at[layer, mine], w[i].at[layer, rows(i, me, h * half[i] + r0, nr)])
        return [pltpu.make_async_copy(a, b, feed_s.at[z, c, slot]) for z, (a, b) in enumerate(zip(src, feed_slot(k), strict=True))]

    exchanged, started = 0, {0: 0, 1: 0}

    def next_exchange():
        nonlocal exchanged
        if exchanged < len(exchanges):
            exchange(exchanged).start()
            exchanged += 1

    def next_term(c):
        if started[c] < len(order[c]):
            term(order[c][started[c]]).start()
            started[c] += 1

    next_term(0)
    next_term(0)
    pl.semaphore_wait(barrier, 3)
    for _ in range(4):
        next_exchange()
    next_term(0)
    next_term(0)

    def tile_of(cols, nr):
        return min(65536 // cols, nr)

    zero = jnp.zeros((8, 128), F32)
    total = (zero,) * 4
    for k, step in enumerate(steps):
        i, layer = units[step.u]
        c = kind[i]
        dst = part(step)
        meet(step)
        term(k).wait()
        more = []
        for stream in step.needs:
            arrive(stream, step)
            more.append(landed(step, stream))
        own = own_rows(k)
        cols = dst.shape[1]
        tile = tile_of(cols, step.nr)

        def body(r, acc, dst=dst, own=own, more=more, cols=cols, tile=tile, squared=not step.send):
            at_rows = pl.ds(pl.multiple_of(r * tile, tile), tile)
            s = own[at_rows, :].astype(F32) + dst[at_rows, :].astype(F32)
            for one in more:
                s = s + one[at_rows, :].astype(F32)
            b = s.astype(BF)
            dst[at_rows, :] = b
            if squared:
                q = b.astype(F32)
                q = q * q
                acc = list(acc)
                for a in range(tile // 8):
                    for z in range(cols // 128):
                        acc[(a + z) % 4] = acc[(a + z) % 4] + q[8 * a : 8 * a + 8, 128 * z : 128 * z + 128]
                acc = tuple(acc)
            return acc

        if step.send:
            lax.fori_loop(0, step.nr // tile, body, ())
            push(k).start()
        else:
            total = lax.fori_loop(0, step.nr // tile, body, total)
            pltpu.make_async_copy(dst, gsum[i].at[layer, pl.ds(step.h * half[i] + step.r0, step.nr)], loc_s.at[0, i]).start()
        next_term(c)
        next_exchange()
        if k == 5:
            for _ in range(RING):
                next_term(1)
        if k == 20:
            for c in (0, 1):
                for z in feed_order[c][: FEED[c]]:
                    for copy in feed(z):
                        copy.start()

    squares[n] = total[0] + total[1] + total[2] + total[3]
    for k in range(1, n):
        remote(squares.at[n], squares.at[me], sq_s.at[0], sq_s.at[1], (me + k) % n).start()
    for i in range(3):
        remote(pair[i], pair[i], d2d_s.at[i], d2d_r.at[0], mate).wait_send()
        remote(land[i], land[i], lk_s.at[i], lk_r.at[0], xnbr).wait_send()
    squares[me] = squares[n]
    others = squares.at[pl.ds(0, n - 1)]
    remote(others, others, sq_s.at[0], sq_s.at[1], xnbr).wait_recv()
    everything = squares[0]
    for k in range(1, n):
        everything = everything + squares[k]
    everything = jnp.sum(jnp.sum(everything, axis=0, keepdims=True), axis=1, keepdims=True)
    factor = jnp.minimum(1.0, 0.5 * lax.rsqrt(everything / count + 1e-30))
    factor_v[...] = jnp.broadcast_to(factor, (8, 128))

    def out(i, layer, device, r0=0, nr=None):
        return whole[i].at[layer, rows(i, device, r0, nr)]

    gathered = [u for u in range(len(units)) if units[u][0] < KEPT]
    sent = [k for k, piece in enumerate(fed) if piece[0] in gathered]

    for k, (u, h, r0, nr) in enumerate(fed):
        i, layer = units[u]
        c = kind[i]
        for copy in feed(k):
            copy.wait()
        mine = pl.ds(h * half[i] + r0, nr)
        dst, src = pair[i].at[DG, layer, mine], pair[i].at[ME, layer, mine]
        mm, vv, ww = feed_slot(k)
        tile = min(32768 // dst.shape[1] if c else 16, nr)

        def body(r, _, dst=dst, src=src, mm=mm, vv=vv, ww=ww, tile=tile):
            at_rows = pl.ds(pl.multiple_of(r * tile, tile), tile)
            grad = src[at_rows, :].astype(F32) * factor_v[0:1, 0:1]
            m_new, v_new = moments(mm[at_rows, :], vv[at_rows, :], grad)
            weight = ww[at_rows, :].astype(F32)
            dst[at_rows, :] = (weight - 0.02 * (m_new * lax.rsqrt(v_new + 1e-8) + 0.1 * weight)).astype(BF)
            return 0

        lax.fori_loop(0, nr // tile, body, 0)
        if i < KEPT:
            here = out(i, layer, me, h * half[i] + r0, nr)
            z = sent.index(k)
            remote(dst, here, own_s.at[0, i], lk_r.at[z], xnbr).start()
            remote(dst, here, own_s.at[1, i], lk_r.at[len(sent) + z], ynbr).start()
            remote(dst, here, own_s.at[2, i], d2d_r.at[z], mate).start()
            pltpu.make_async_copy(dst, here, loc_s.at[1, i]).start()
        else:
            remote(dst, mates[h].at[layer], end_s.at[0, h], end_r.at[0, h], mate).start()
            pltpu.make_async_copy(dst, ends[h].at[layer], loc_s.at[2, h]).start()
            tail = half[i] // CUT
            pltpu.make_async_copy(dst.at[pl.ds(0, half[i] - tail)], parts[h].at[layer], loc_s.at[3, h]).start()
        if feed_at[k] + FEED[c] < len(feed_order[c]):
            for copy in feed(feed_order[c][feed_at[k] + FEED[c]]):
                copy.start()

    relays = [(u, h, block) for u in gathered for h in range(2) for block in (XN, YN, DG)]

    def relay(u, h, block):
        i, layer = units[u]
        here = out(i, layer, owner(block, core), h * half[i], half[i])
        remote(here, here, rel_s.at[block - 1, i], d2d_r.at[len(sent) + relays.index((u, h, block))], mate).start()

    def forward_sem(u, h):
        return lk_r.at[2 * len(sent) + 2 * u + h]

    def onward(u, h, block, device):
        i, layer = units[u]
        here = out(i, layer, owner(block, core), h * half[i], half[i])
        remote(here, here, fwd_s.at[h, i], forward_sem(u, h), device).start()

    def from_link(u, h, which):
        i, layer = units[u]
        for z, k in enumerate(sent):
            if fed[k][:2] == (u, h):
                there = out(i, layer, owner((XN, YN)[which], core), h * half[i] + fed[k][2], fed[k][3])
                remote(there, there, own_s.at[0, 0], lk_r.at[which * len(sent) + z], xnbr).wait_recv()

    for u in gathered:
        from_link(u, 0, 0)
        onward(u, 0, XN, ynbr)
        relay(u, 0, XN)
        from_link(u, 1, 1)
        onward(u, 1, YN, xnbr)
        relay(u, 1, YN)
        from_link(u, 0, 1)
        relay(u, 0, YN)
        from_link(u, 1, 0)
        relay(u, 1, XN)

    for u, (i, layer) in enumerate(units):
        if i >= KEPT:
            tail = half[i] // CUT
            for h in range(2):
                src = pair[i].at[DG, layer, pl.ds((h + 1) * half[i] - tail, tail)]
                remote(src, tails[h].at[layer], end_s.at[1, h], end_r.at[1, h], across[h]).start()

    for u in gathered:
        i, layer = units[u]
        for h in range(2):
            there = out(i, layer, owner(DG, core), h * half[i], half[i])
            remote(there, there, fwd_s.at[0, 0], forward_sem(u, h), xnbr).wait_recv()
            relay(u, h, DG)

    for i in range(3):
        pltpu.make_async_copy(gsum[i], gsum[i], loc_s.at[0, i]).wait()
    for i in range(KEPT):
        block, part_of = whole[i].at[:, pl.ds(0, 2 * half[i])], whole[i].at[:, pl.ds(0, half[i])]
        pltpu.make_async_copy(block, block, loc_s.at[1, i]).wait()
        for z in range(3):
            remote(block, block, own_s.at[z, i], lk_r.at[0], xnbr).wait_send()
        for h in range(2):
            remote(part_of, part_of, fwd_s.at[h, i], lk_r.at[0], xnbr).wait_send()
    for h in range(2):
        pltpu.make_async_copy(ends[h], ends[h], loc_s.at[2, h]).wait()
        pltpu.make_async_copy(parts[h], parts[h], loc_s.at[3, h]).wait()
        both = remote(mates[h], mates[h], end_s.at[0, h], end_r.at[0, h], mate)
        both.wait_send()
        both.wait_recv()
    remote(others, others, sq_s.at[0], sq_s.at[1], xnbr).wait_send()
    for z, k in enumerate(sent):
        u, h, r0, nr = fed[k]
        i, layer = units[u]
        there = out(i, layer, mate, h * half[i] + r0, nr)
        remote(there, there, own_s.at[0, 0], d2d_r.at[z], mate).wait_recv()
    done = pltpu.make_async_copy(factor_v, factor_ref, loc_s.at[0, 0])
    done.start()
    done.wait()
    for z, (u, h, block) in enumerate(relays):
        i, layer = units[u]
        there = out(i, layer, owner(block, 1 - core), h * half[i], half[i])
        remote(there, there, rel_s.at[0, 0], d2d_r.at[len(sent) + z], mate).wait_recv()
    for i in range(KEPT):
        block = whole[i].at[:, pl.ds(0, 2 * half[i])]
        for z in range(3):
            remote(block, block, rel_s.at[z, i], d2d_r.at[0], mate).wait_send()
    for h in range(2):
        both = remote(tails[h], tails[h], end_s.at[1, h], end_r.at[1, h], xnbr)
        both.wait_send()
        both.wait_recv()


class Step(NamedTuple):
    send: bool
    block: int
    u: int
    h: int
    r0: int
    nr: int
    stream: int | None
    needs: tuple


def geometry(land, layers):
    return [(i, layer) for i in range(3) for layer in range(layers)], (0, 0, 1), [p.shape[2] for p in land]


def cuts(size, shares):
    at = 0
    for share in shares:
        yield at, size * share // 4
        at += size * share // 4


def rs_steps(units, half):
    steps = []
    last = len(units) - 1

    def add(send, u, shares, *two):
        for r0, nr in cuts(half[units[u][0]], shares):
            steps.extend(Step(send, block, u, h, r0, nr, stream, needs) for block, h, stream, needs in two)

    for u in range(last + 1):
        add(True, u, (1, 1, 2) if u == 0 else (4,), (DG, 0, XD, ()), (DG, 1, YD, ()))
    for u in range(last + 1):
        add(True, u, (4,), (XN, 0, XO, ()), (YN, 1, YO, ()))
    for u in range(last + 1):
        add(True, u, (2, 1, 1) if u == last else (4,), (YN, 0, YT, (XD,)), (XN, 1, XT, (YD,)))
    for u in range(last + 1):
        add(False, u, (2, 1, 1) if u == last else (4,), (ME, 0, None, (XO, YT)), (ME, 1, None, (YO, XT)))
    return steps


def exchange_list(steps, half, units):
    first = [(s.block, s.u, s.h * half[units[s.u][0]] + s.r0, s.nr) for s in steps if s.block == DG]
    return first + [(block, u, 0, 2 * half[i]) for two in ((XN, YN), (ME,)) for u, (i, _) in enumerate(units) for block in two]


def make_order(units, half):
    pieces = []
    for u, (i, _) in enumerate(units):
        for r0, nr in cuts(half[i], (1, 3) if u == 0 else (4,)):
            pieces += [(u, 0, r0, nr), (u, 1, r0, nr)]
    return pieces


def cost(size):
    return pl.CostEstimate(flops=size * 12, bytes_accessed=size, transcendentals=0)


def place_kernel(*refs, spots, half, moves, grown):
    k = len(spots)
    pieces_in, whole_in = refs[:k], refs[k : k + moves]
    outs = refs[k + moves + grown :][: moves + 1]
    scratch = refs[k + 2 * moves + grown + 1 :]
    bufs, moved, in_s, out_s = scratch[:k], scratch[k : k + moves], scratch[-2], scratch[-1]
    _, core, owner = neighbours()
    jobs = []
    for a in range(moves):
        layers, height = whole_in[a].shape[:2]
        size = height // 4
        for layer in range(layers):
            for p in range(4):
                at = pl.ds(p * size, size)
                jobs.append((whole_in[a].at[layer, at], moved[a].at[layer, at], outs[a].at[layer, at]))
    for z in range(k):
        block, other, h, r0 = spots[z]
        start = (2 * owner(block, 1 - core if other else core) + h) * half + r0
        at = pl.ds(pl.multiple_of(start, 16), pieces_in[z].shape[1])
        jobs.append((pieces_in[z], bufs[z], outs[moves].at[:, at]))
    loads = [functools.partial(pltpu.make_async_copy, src, buf, in_s.at[j]) for j, (src, buf, _) in enumerate(jobs)]
    stores = [functools.partial(pltpu.make_async_copy, buf, dst, out_s.at[j]) for j, (_, buf, dst) in enumerate(jobs)]
    for load in loads:
        load().start()
    for load, store in zip(loads, stores, strict=True):
        load().wait()
        store().start()
    for store in stores:
        store().wait()


def place(pieces, shape, half, into=None, moves=()):
    spots, arrays = zip(*pieces)
    grown = into is not None
    size = sum(a.size * 4 for a in (*arrays, *moves))
    jobs = len(arrays) + sum(4 * a.shape[0] for a in moves)
    like = [jax.ShapeDtypeStruct(a.shape, a.dtype) for a in moves] + [jax.ShapeDtypeStruct(shape, arrays[0].dtype)]
    in_hbm = pl.BlockSpec(memory_space=pltpu.HBM)
    out = pl.pallas_call(
        functools.partial(place_kernel, spots=spots, half=half, moves=len(moves), grown=int(grown)),
        out_shape=like,
        in_specs=[in_hbm] * (len(arrays) + len(moves) + grown),
        out_specs=[in_hbm] * len(like),
        scratch_shapes=[pltpu.VMEM(a.shape, a.dtype) for a in (*arrays, *moves)] + [pltpu.SemaphoreType.DMA((jobs,))] * 2,
        input_output_aliases={len(arrays) + len(moves): len(moves)} if grown else {},
        compiler_params=pltpu.CompilerParams(vmem_limit_bytes=67043328),
        cost_estimate=cost(size),
    )(*arrays, *moves, *((into,) if grown else ()))
    return out if moves else out[0]


def fresh_kernel(*refs):
    m, v, g, factor_ref, m_new, v_new = refs[:3], refs[3:6], refs[6:9], refs[9], refs[10:13], refs[13:16]
    bufs, in_s, out_s = refs[16:25], refs[25], refs[26]
    pieces = []
    for i in range(3):
        layers, height = m[i].shape[:2]
        pieces += [(i, layer, p * (height // 2), height // 2) for layer in range(layers) for p in range(2)]

    def loads(z):
        i, layer, r0, nr = pieces[z]
        at_rows = pl.ds(r0, nr)
        return [pltpu.make_async_copy(a[i].at[layer, at_rows], bufs[3 * t + i].at[layer, at_rows], in_s.at[t, z]) for t, a in enumerate((m, v, g))]

    def stores(z):
        i, layer, r0, nr = pieces[z]
        at_rows = pl.ds(r0, nr)
        return [pltpu.make_async_copy(bufs[3 * t + i].at[layer, at_rows], a[i].at[layer, at_rows], out_s.at[t, z]) for t, a in enumerate((m_new, v_new))]

    for z in range(len(pieces)):
        for copy in loads(z):
            copy.start()
    for z, (i, layer, r0, nr) in enumerate(pieces):
        for copy in loads(z):
            copy.wait()
        mm, vv, gg = (bufs[3 * t + i].at[layer] for t in range(3))
        tile = 65536 // mm.shape[1]

        def body(r, _, mm=mm, vv=vv, gg=gg, r0=r0, tile=tile):
            at_rows = pl.ds(pl.multiple_of(r0 + r * tile, tile), tile)
            grad = gg[at_rows, :].astype(F32) * factor_ref[0:1, 0:1]
            mm[at_rows, :], vv[at_rows, :] = moments(mm[at_rows, :], vv[at_rows, :], grad)
            return 0

        lax.fori_loop(0, nr // tile, body, 0)
        for copy in stores(z):
            copy.start()
    for z in range(len(pieces)):
        for copy in stores(z):
            copy.wait()


def fresh(m, v, sums, factor):
    pieces = 2 * sum(one.shape[0] for one in m)
    size = sum(one.size * 18 for one in m)
    dma = pltpu.SemaphoreType.DMA
    any_space = pl.BlockSpec(memory_space=pltpu.HBM)
    out = pl.pallas_call(
        fresh_kernel,
        name="fresh",
        out_shape=[jax.ShapeDtypeStruct(one.shape, F32) for one in (*m, *v)],
        in_specs=[any_space] * 9 + [pl.BlockSpec(memory_space=pltpu.VMEM)],
        out_specs=[any_space] * 6,
        scratch_shapes=[pltpu.VMEM(one.shape, one.dtype) for one in (*m, *v, *sums)] + [dma((3, pieces)), dma((2, pieces))],
        compiler_params=pltpu.CompilerParams(vmem_limit_bytes=67043328),
        cost_estimate=cost(size),
    )(*m, *v, *sums, factor)
    return out[:3], out[3:]


def solution(mesh):
    n = mesh.shape["dp"]

    def step(*arrays):
        terms, weights, m, v = (arrays[i : i + 3] for i in (0, 3, 6, 9))
        layers = weights[0].shape[0]
        blocks = [(one.shape[1] // 2, one.shape[2]) for one in m]
        kinds = (blocks[0], blocks[2])
        count = float(n * sum(one.size for one in m))
        dma = pltpu.SemaphoreType.DMA
        units = [(i, layer) for i in range(3) for layer in range(layers)]
        halves = [b[0] for b in blocks]
        steps = rs_steps(units, halves)
        pieces = sum(units[piece[0]][0] < KEPT for piece in make_order(units, halves))
        swaps = max(len(exchange_list(steps, halves, units)), pieces + 6 * KEPT * layers)
        hops = max(sum(one.send for one in steps), 2 * pieces + 2 * KEPT * layers)
        any_space = pl.BlockSpec(memory_space=pl.ANY)
        half, cols = blocks[KEPT]
        tail = half // CUT
        shapes = [one.shape for one in weights[:KEPT]] + [(layers, half, cols)] * 4 + [(layers, half - tail, cols)] * 2 + [(layers, tail, cols)] * 2
        shapes += [one.shape for one in m]
        out = pl.pallas_call(
            functools.partial(kernel, n=n, layers=layers, count=count),
            name="step",
            out_shape=[jax.ShapeDtypeStruct(shape, BF) for shape in shapes] + [jax.ShapeDtypeStruct((8, 128), F32)],
            in_specs=[any_space] * 12,
            out_specs=[any_space] * (len(shapes) + 1),
            scratch_shapes=[pltpu.VMEM((4, layers, 2 * b[0], b[1]), BF) for b in blocks]
            + [pltpu.VMEM((6, layers, *b), BF) for b in blocks]
            + [pltpu.VMEM((RING, *b), BF) for b in kinds]
            + [pltpu.VMEM((size, *b), F32) for size, b in zip(FEED, kinds, strict=True)] * 2
            + [pltpu.VMEM((size, *b), BF) for size, b in zip(FEED, kinds, strict=True)]
            + [pltpu.VMEM((n + 1, 8, 128), F32), pltpu.VMEM((8, 128), F32)]
            + [dma((3,)), dma((swaps,)), dma((3,)), dma((hops,)), dma((2, RING)), dma((3, 2, max(FEED)))]
            + [dma((2,)), dma((3, KEPT)), dma((2, KEPT)), dma((3, KEPT)), dma((4, 3)), dma((2, 2)), dma((2, 2))],
            compiler_params=pltpu.CompilerParams(collective_id=0, has_side_effects=True, vmem_limit_bytes=67043328),
        )(*terms, *weights, *m, *v)
        kept, (low, high), (m_low, m_high), (low_a, high_a), (x_low_b, y_high_b) = (out[i : i + 2] for i in range(0, 10, 2))
        sums, factor = out[10:13], out[13]

        def hop(a, flip):
            return lax.ppermute(a, "dp", [(i, i ^ flip) for i in range(n)])

        barrier = lax.optimization_barrier
        x, y, mate = n // 2, n // 4, 1
        x_low_a, y_high_a = hop(low_a, x), hop(high_a, y)
        x_high, y_low = hop(high, x), hop(low, y)
        mx_b, my_b = hop(x_low_b, mate), hop(y_high_b, mate)
        new_m, new_v = fresh(m, v, sums, factor)
        x_low_a, y_high_a, new_m, new_v = barrier((x_low_a, y_high_a, new_m, new_v))
        d_low_a, d_high_a = hop(x_low_a, y), hop(y_high_a, x)
        d_low_b, d_high_b = hop(x_low_b, y), hop(y_high_b, x)
        mx_a, my_a = hop(x_low_a, mate), hop(y_high_a, mate)
        shape, b = weights[KEPT].shape, half - tail
        first = [((ME, 0, 0, 0), low), ((ME, 0, 1, 0), high), ((ME, 1, 0, 0), m_low), ((ME, 1, 1, 0), m_high)]
        first += [((XN, 0, 0, 0), x_low_a), ((YN, 0, 1, 0), y_high_a), ((XN, 0, 0, b), x_low_b), ((YN, 0, 1, b), y_high_b)]
        first += [((XN, 1, 0, b), mx_b), ((YN, 1, 1, b), my_b)]
        gate, up, down = place(first, shape, half, moves=kept)
        x_high, y_low, gate, up, down = barrier((x_high, y_low, gate, up, down))
        mx_high, my_low = hop(x_high, mate), hop(y_low, mate)
        then = [((XN, 1, 0, 0), mx_a), ((YN, 1, 1, 0), my_a), ((XN, 0, 1, 0), x_high), ((YN, 0, 0, 0), y_low)]
        down = place(then, shape, half, down)
        d_low_a, d_high_a, down = barrier((d_low_a, d_high_a, down))
        md_low_a, md_high_a = hop(d_low_a, mate), hop(d_high_a, mate)
        more = [((XN, 1, 1, 0), mx_high), ((YN, 1, 0, 0), my_low), ((DG, 0, 0, 0), d_low_a), ((DG, 0, 1, 0), d_high_a)]
        down = place(more, shape, half, down)
        d_low_b, d_high_b, down = barrier((d_low_b, d_high_b, down))
        md_low_b, md_high_b = hop(d_low_b, mate), hop(d_high_b, mate)
        down = place([((DG, 1, 0, 0), md_low_a), ((DG, 1, 1, 0), md_high_a)], shape, half, down)
        late_b = [((DG, 0, 0, b), d_low_b), ((DG, 0, 1, b), d_high_b), ((DG, 1, 0, b), md_low_b), ((DG, 1, 1, b), md_high_b)]
        down = place(late_b, shape, half, down)
        return (gate, up, down, *new_m, *new_v)

    all_of, cut = P(None, None, None), P(None, "dp", None)
    return jax.shard_map(
        step,
        mesh=mesh,
        in_specs=(P(("rep", "dp"), None, None, None),) * 3 + (all_of,) * 3 + (cut,) * 6,
        out_specs=(P("rep", None, None),) * 3 + (P("rep", "dp", None),) * 6,
        check_vma=False,
    )
```

```python
import functools
from typing import NamedTuple

import jax
import jax.numpy as jnp
from jax import lax
from jax.experimental import pallas as pl
from jax.experimental.pallas import tpu as pltpu
from jax.sharding import PartitionSpec as P


BF, F32 = jnp.bfloat16, jnp.float32
RING = 4
FEED = (3, 2)
KEPT = 2
CUT = 4
ME, XN, YN, DG = range(4)
XD, XO, XT, YD, YO, YT = range(6)


def moments(m, v, g):
    return 0.9 * m + 0.1 * g, 0.95 * v + 0.05 * g * g


def neighbours():
    me = lax.axis_index("dp")
    core, chip = me % 2, me // 2
    cy, cx = chip % 2, chip // 2
    owner = lambda block, c: 4 * (1 - cx if block in (XN, DG) else cx) + 2 * (1 - cy if block in (YN, DG) else cy) + c
    return me, core, owner


def kernel(*refs, n, layers, count):
    it = iter(refs)
    take = lambda k: [next(it) for _ in range(k)]
    g, w, m, v = take(3), take(3), take(3), take(3)
    whole, ends, mates, parts, tails, gsum, factor_ref = take(KEPT), take(2), take(2), take(2), take(2), take(3), next(it)
    pair, land = take(3), take(3)
    gring, mring, vring, wring = take(2), take(2), take(2), take(2)
    squares, factor_v = take(2)
    d2d_s, d2d_r, lk_s, lk_r, ring_s, feed_s = take(6)
    sq_s, own_s, fwd_s, rel_s, loc_s, end_s, end_r = take(7)

    me, core, owner = neighbours()
    mate, xnbr, ynbr = owner(ME, 1 - core), owner(XN, core), owner(YN, core)
    across = (xnbr, ynbr)

    def remote(src, dst, s, r, device):
        return pltpu.make_async_remote_copy(
            src_ref=src, dst_ref=dst, send_sem=s, recv_sem=r, device_id={"dp": device}, device_id_type=pl.DeviceIdType.MESH
        )

    barrier = pltpu.get_barrier_semaphore()
    for device in (mate, xnbr, ynbr):
        pl.semaphore_signal(barrier, inc=1, device_id={"dp": device}, device_id_type=pl.DeviceIdType.MESH)

    units, kind, half = geometry(land, layers)

    def rows(i, device, r0=0, nr=None):
        return pl.ds(pl.multiple_of(device * (2 * half[i]) + r0, 16), 2 * half[i] if nr is None else nr)

    steps = rs_steps(units, half)
    exchanges = exchange_list(steps, half, units)

    def part(step):
        return pair[units[step.u][0]].at[step.block, units[step.u][1], pl.ds(step.h * half[units[step.u][0]] + step.r0, step.nr)]

    def exchange(z):
        block, u, r0, nr = exchanges[z]
        i, layer = units[u]
        src = g[i].at[0, layer, rows(i, owner(block, 1 - core), r0, nr)]
        return remote(src, pair[i].at[block, layer, pl.ds(r0, nr)], d2d_s.at[i], d2d_r.at[z], mate)

    order = {c: [k for k, step in enumerate(steps) if kind[units[step.u][0]] == c] for c in (0, 1)}
    place_of = {k: (c, p) for c in order for p, k in enumerate(order[c])}

    def own_rows(k):
        c, p = place_of[k]
        return gring[c].at[p % RING, pl.ds(0, steps[k].nr)]

    def term(k):
        step = steps[k]
        i, layer = units[step.u]
        c, p = place_of[k]
        src = g[i].at[0, layer, rows(i, owner(step.block, core), step.h * half[i] + step.r0, step.nr)]
        return pltpu.make_async_copy(src, own_rows(k), ring_s.at[c, p % RING])

    def landed(step, stream):
        i, layer = units[step.u]
        return land[i].at[stream, layer, pl.ds(step.r0, step.nr)]

    def push(k):
        step = steps[k]
        return remote(part(step), landed(step, step.stream), lk_s.at[units[step.u][0]], lk_r.at[k], across[step.stream >= YD])

    seen, met = set(), set()

    def arrive(stream, step):
        for k, other in enumerate(steps):
            overlap = other.r0 < step.r0 + step.nr and step.r0 < other.r0 + other.nr
            if other.send and other.stream == stream and other.u == step.u and overlap and k not in seen:
                seen.add(k)
                dst = landed(other, stream)
                remote(dst, dst, lk_s.at[0], lk_r.at[k], xnbr).wait_recv()

    def meet(step):
        first = step.h * half[units[step.u][0]] + step.r0
        for z, (block, u, r0, nr) in enumerate(exchanges):
            if block == step.block and u == step.u and r0 < first + step.nr and first < r0 + nr and z not in met:
                met.add(z)
                i, layer = units[u]
                dst = pair[i].at[block, layer, pl.ds(r0, nr)]
                remote(dst, dst, d2d_s.at[0], d2d_r.at[z], mate).wait_recv()

    fed = make_order(units, half)
    feed_order = {c: [k for k, piece in enumerate(fed) if kind[units[piece[0]][0]] == c] for c in (0, 1)}
    feed_at = {k: p for c in (0, 1) for p, k in enumerate(feed_order[c])}

    def feed_slot(k):
        c = kind[units[fed[k][0]][0]]
        return [ring[c].at[feed_at[k] % FEED[c], pl.ds(0, fed[k][3])] for ring in (mring, vring, wring)]

    def feed(k):
        u, h, r0, nr = fed[k]
        i, layer = units[u]
        c = kind[i]
        slot = feed_at[k] % FEED[c]
        mine = pl.ds(h * half[i] + r0, nr)
        src = (m[i].at[layer, mine], v[i].at[layer, mine], w[i].at[layer, rows(i, me, h * half[i] + r0, nr)])
        return [pltpu.make_async_copy(a, b, feed_s.at[z, c, slot]) for z, (a, b) in enumerate(zip(src, feed_slot(k), strict=True))]

    exchanged, started = 0, {0: 0, 1: 0}

    def next_exchange():
        nonlocal exchanged
        if exchanged < len(exchanges):
            exchange(exchanged).start()
            exchanged += 1

    def next_term(c):
        if started[c] < len(order[c]):
            term(order[c][started[c]]).start()
            started[c] += 1

    next_term(0)
    next_term(0)
    pl.semaphore_wait(barrier, 3)
    for _ in range(4):
        next_exchange()
    next_term(0)
    next_term(0)

    def tile_of(cols, nr):
        return min(65536 // cols, nr)

    zero = jnp.zeros((8, 128), F32)
    total = (zero,) * 4
    for k, step in enumerate(steps):
        i, layer = units[step.u]
        c = kind[i]
        dst = part(step)
        meet(step)
        term(k).wait()
        more = []
        for stream in step.needs:
            arrive(stream, step)
            more.append(landed(step, stream))
        own = own_rows(k)
        cols = dst.shape[1]
        tile = tile_of(cols, step.nr)

        def body(r, acc, dst=dst, own=own, more=more, cols=cols, tile=tile, squared=not step.send):
            at_rows = pl.ds(pl.multiple_of(r * tile, tile), tile)
            s = own[at_rows, :].astype(F32) + dst[at_rows, :].astype(F32)
            for one in more:
                s = s + one[at_rows, :].astype(F32)
            b = s.astype(BF)
            dst[at_rows, :] = b
            if squared:
                q = b.astype(F32)
                q = q * q
                acc = list(acc)
                for a in range(tile // 8):
                    for z in range(cols // 128):
                        acc[(a + z) % 4] = acc[(a + z) % 4] + q[8 * a : 8 * a + 8, 128 * z : 128 * z + 128]
                acc = tuple(acc)
            return acc

        if step.send:
            lax.fori_loop(0, step.nr // tile, body, ())
            push(k).start()
        else:
            total = lax.fori_loop(0, step.nr // tile, body, total)
            pltpu.make_async_copy(dst, gsum[i].at[layer, pl.ds(step.h * half[i] + step.r0, step.nr)], loc_s.at[0, i]).start()
        next_term(c)
        next_exchange()
        if k == 5:
            for _ in range(RING):
                next_term(1)
        if k == 20:
            for c in (0, 1):
                for z in feed_order[c][: FEED[c]]:
                    for copy in feed(z):
                        copy.start()

    squares[n] = total[0] + total[1] + total[2] + total[3]
    for k in range(1, n):
        remote(squares.at[n], squares.at[me], sq_s.at[0], sq_s.at[1], (me + k) % n).start()
    for i in range(3):
        remote(pair[i], pair[i], d2d_s.at[i], d2d_r.at[0], mate).wait_send()
        remote(land[i], land[i], lk_s.at[i], lk_r.at[0], xnbr).wait_send()
    squares[me] = squares[n]
    others = squares.at[pl.ds(0, n - 1)]
    remote(others, others, sq_s.at[0], sq_s.at[1], xnbr).wait_recv()
    everything = squares[0]
    for k in range(1, n):
        everything = everything + squares[k]
    everything = jnp.sum(jnp.sum(everything, axis=0, keepdims=True), axis=1, keepdims=True)
    factor = jnp.minimum(1.0, 0.5 * lax.rsqrt(everything / count + 1e-30))
    factor_v[...] = jnp.broadcast_to(factor, (8, 128))

    def out(i, layer, device, r0=0, nr=None):
        return whole[i].at[layer, rows(i, device, r0, nr)]

    gathered = [u for u in range(len(units)) if units[u][0] < KEPT]
    sent = [k for k, piece in enumerate(fed) if piece[0] in gathered]

    for k, (u, h, r0, nr) in enumerate(fed):
        i, layer = units[u]
        c = kind[i]
        for copy in feed(k):
            copy.wait()
        mine = pl.ds(h * half[i] + r0, nr)
        dst, src = pair[i].at[DG, layer, mine], pair[i].at[ME, layer, mine]
        mm, vv, ww = feed_slot(k)
        tile = min(32768 // dst.shape[1] if c else 16, nr)

        def body(r, _, dst=dst, src=src, mm=mm, vv=vv, ww=ww, tile=tile):
            at_rows = pl.ds(pl.multiple_of(r * tile, tile), tile)
            grad = src[at_rows, :].astype(F32) * factor_v[0:1, 0:1]
            m_new, v_new = moments(mm[at_rows, :], vv[at_rows, :], grad)
            weight = ww[at_rows, :].astype(F32)
            dst[at_rows, :] = (weight - 0.02 * (m_new * lax.rsqrt(v_new + 1e-8) + 0.1 * weight)).astype(BF)
            return 0

        lax.fori_loop(0, nr // tile, body, 0)
        if i < KEPT:
            here = out(i, layer, me, h * half[i] + r0, nr)
            z = sent.index(k)
            remote(dst, here, own_s.at[0, i], lk_r.at[z], xnbr).start()
            remote(dst, here, own_s.at[1, i], lk_r.at[len(sent) + z], ynbr).start()
            remote(dst, here, own_s.at[2, i], d2d_r.at[z], mate).start()
            pltpu.make_async_copy(dst, here, loc_s.at[1, i]).start()
        else:
            remote(dst, mates[h].at[layer], end_s.at[0, h], end_r.at[0, h], mate).start()
            pltpu.make_async_copy(dst, ends[h].at[layer], loc_s.at[2, h]).start()
            tail = half[i] // CUT
            pltpu.make_async_copy(dst.at[pl.ds(0, half[i] - tail)], parts[h].at[layer], loc_s.at[3, h]).start()
        if feed_at[k] + FEED[c] < len(feed_order[c]):
            for copy in feed(feed_order[c][feed_at[k] + FEED[c]]):
                copy.start()

    relays = [(u, h, block) for u in gathered for h in range(2) for block in (XN, YN, DG)]

    def relay(u, h, block):
        i, layer = units[u]
        here = out(i, layer, owner(block, core), h * half[i], half[i])
        remote(here, here, rel_s.at[block - 1, i], d2d_r.at[len(sent) + relays.index((u, h, block))], mate).start()

    def forward_sem(u, h):
        return lk_r.at[2 * len(sent) + 2 * u + h]

    def onward(u, h, block, device):
        i, layer = units[u]
        here = out(i, layer, owner(block, core), h * half[i], half[i])
        remote(here, here, fwd_s.at[h, i], forward_sem(u, h), device).start()

    def from_link(u, h, which):
        i, layer = units[u]
        for z, k in enumerate(sent):
            if fed[k][:2] == (u, h):
                there = out(i, layer, owner((XN, YN)[which], core), h * half[i] + fed[k][2], fed[k][3])
                remote(there, there, own_s.at[0, 0], lk_r.at[which * len(sent) + z], xnbr).wait_recv()

    for u in gathered:
        from_link(u, 0, 0)
        onward(u, 0, XN, ynbr)
        relay(u, 0, XN)
        from_link(u, 1, 1)
        onward(u, 1, YN, xnbr)
        relay(u, 1, YN)
        from_link(u, 0, 1)
        relay(u, 0, YN)
        from_link(u, 1, 0)
        relay(u, 1, XN)

    for u, (i, layer) in enumerate(units):
        if i >= KEPT:
            tail = half[i] // CUT
            for h in range(2):
                src = pair[i].at[DG, layer, pl.ds((h + 1) * half[i] - tail, tail)]
                remote(src, tails[h].at[layer], end_s.at[1, h], end_r.at[1, h], across[h]).start()

    for u in gathered:
        i, layer = units[u]
        for h in range(2):
            there = out(i, layer, owner(DG, core), h * half[i], half[i])
            remote(there, there, fwd_s.at[0, 0], forward_sem(u, h), xnbr).wait_recv()
            relay(u, h, DG)

    for i in range(3):
        pltpu.make_async_copy(gsum[i], gsum[i], loc_s.at[0, i]).wait()
    for i in range(KEPT):
        block, part_of = whole[i].at[:, pl.ds(0, 2 * half[i])], whole[i].at[:, pl.ds(0, half[i])]
        pltpu.make_async_copy(block, block, loc_s.at[1, i]).wait()
        for z in range(3):
            remote(block, block, own_s.at[z, i], lk_r.at[0], xnbr).wait_send()
        for h in range(2):
            remote(part_of, part_of, fwd_s.at[h, i], lk_r.at[0], xnbr).wait_send()
    for h in range(2):
        pltpu.make_async_copy(ends[h], ends[h], loc_s.at[2, h]).wait()
        pltpu.make_async_copy(parts[h], parts[h], loc_s.at[3, h]).wait()
        both = remote(mates[h], mates[h], end_s.at[0, h], end_r.at[0, h], mate)
        both.wait_send()
        both.wait_recv()
    remote(others, others, sq_s.at[0], sq_s.at[1], xnbr).wait_send()
    for z, k in enumerate(sent):
        u, h, r0, nr = fed[k]
        i, layer = units[u]
        there = out(i, layer, mate, h * half[i] + r0, nr)
        remote(there, there, own_s.at[0, 0], d2d_r.at[z], mate).wait_recv()
    done = pltpu.make_async_copy(factor_v, factor_ref, loc_s.at[0, 0])
    done.start()
    done.wait()
    for z, (u, h, block) in enumerate(relays):
        i, layer = units[u]
        there = out(i, layer, owner(block, 1 - core), h * half[i], half[i])
        remote(there, there, rel_s.at[0, 0], d2d_r.at[len(sent) + z], mate).wait_recv()
    for i in range(KEPT):
        block = whole[i].at[:, pl.ds(0, 2 * half[i])]
        for z in range(3):
            remote(block, block, rel_s.at[z, i], d2d_r.at[0], mate).wait_send()
    for h in range(2):
        both = remote(tails[h], tails[h], end_s.at[1, h], end_r.at[1, h], xnbr)
        both.wait_send()
        both.wait_recv()


class Step(NamedTuple):
    send: bool
    block: int
    u: int
    h: int
    r0: int
    nr: int
    stream: int | None
    needs: tuple


def geometry(land, layers):
    return [(i, layer) for i in range(3) for layer in range(layers)], (0, 0, 1), [p.shape[2] for p in land]


def cuts(size, shares):
    at = 0
    for share in shares:
        yield at, size * share // 4
        at += size * share // 4


def rs_steps(units, half):
    steps = []
    last = len(units) - 1

    def add(send, u, shares, *two):
        for r0, nr in cuts(half[units[u][0]], shares):
            steps.extend(Step(send, block, u, h, r0, nr, stream, needs) for block, h, stream, needs in two)

    for u in range(last + 1):
        add(True, u, (1, 3) if u == 0 else (4,), (DG, 0, XD, ()), (DG, 1, YD, ()))
    for u in range(last + 1):
        add(True, u, (4,), (XN, 0, XO, ()), (YN, 1, YO, ()))
    for u in range(last + 1):
        add(True, u, (3, 1) if u == last else (4,), (YN, 0, YT, (XD,)), (XN, 1, XT, (YD,)))
    for u in range(last + 1):
        add(False, u, (3, 1) if u == last else (4,), (ME, 0, None, (XO, YT)), (ME, 1, None, (YO, XT)))
    return steps


def exchange_list(steps, half, units):
    first = [(s.block, s.u, s.h * half[units[s.u][0]] + s.r0, s.nr) for s in steps if s.block == DG]
    return first + [(block, u, 0, 2 * half[i]) for two in ((XN, YN), (ME,)) for u, (i, _) in enumerate(units) for block in two]


def make_order(units, half):
    pieces = []
    for u, (i, _) in enumerate(units):
        for r0, nr in cuts(half[i], (1, 3) if u == 0 else (4,)):
            pieces += [(u, 0, r0, nr), (u, 1, r0, nr)]
    return pieces


def cost(size):
    return pl.CostEstimate(flops=size * 12, bytes_accessed=size, transcendentals=0)


def place_kernel(*refs, spots, half, moves, grown):
    k = len(spots)
    pieces_in, whole_in = refs[:k], refs[k : k + moves]
    outs = refs[k + moves + grown :][: moves + 1]
    scratch = refs[k + 2 * moves + grown + 1 :]
    bufs, moved, in_s, out_s = scratch[:k], scratch[k : k + moves], scratch[-2], scratch[-1]
    _, core, owner = neighbours()
    jobs = []
    for a in range(moves):
        layers, height = whole_in[a].shape[:2]
        size = height // 4
        for layer in range(layers):
            for p in range(4):
                at = pl.ds(p * size, size)
                jobs.append((whole_in[a].at[layer, at], moved[a].at[layer, at], outs[a].at[layer, at]))
    for z in range(k):
        block, other, h, r0 = spots[z]
        start = (2 * owner(block, 1 - core if other else core) + h) * half + r0
        at = pl.ds(pl.multiple_of(start, 16), pieces_in[z].shape[1])
        jobs.append((pieces_in[z], bufs[z], outs[moves].at[:, at]))
    loads = [functools.partial(pltpu.make_async_copy, src, buf, in_s.at[j]) for j, (src, buf, _) in enumerate(jobs)]
    each = (len(jobs) - k) // moves if moves else 1
    done = [j // each if j < len(jobs) - k else moves + j - (len(jobs) - k) for j in range(len(jobs))]
    stores = [functools.partial(pltpu.make_async_copy, buf, dst, out_s.at[z]) for z, (_, buf, dst) in zip(done, jobs, strict=True)]
    for load in loads:
        load().start()
    for load, store in zip(loads, stores, strict=True):
        load().wait()
        store().start()
    for a in range(moves):
        pltpu.make_async_copy(moved[a], outs[a], out_s.at[a]).wait()
    for store in stores[len(jobs) - k :]:
        store().wait()


def place(pieces, shape, half, into=None, moves=()):
    spots, arrays = zip(*pieces)
    grown = into is not None
    size = sum(a.size * 4 for a in (*arrays, *moves))
    jobs = len(arrays) + sum(4 * a.shape[0] for a in moves)
    like = [jax.ShapeDtypeStruct(a.shape, a.dtype) for a in moves] + [jax.ShapeDtypeStruct(shape, arrays[0].dtype)]
    in_hbm = pl.BlockSpec(memory_space=pltpu.HBM)
    out = pl.pallas_call(
        functools.partial(place_kernel, spots=spots, half=half, moves=len(moves), grown=int(grown)),
        out_shape=like,
        in_specs=[in_hbm] * (len(arrays) + len(moves) + grown),
        out_specs=[in_hbm] * len(like),
        scratch_shapes=[pltpu.VMEM(a.shape, a.dtype) for a in (*arrays, *moves)] + [pltpu.SemaphoreType.DMA((jobs,)), pltpu.SemaphoreType.DMA((len(arrays) + len(moves),))],
        input_output_aliases={len(arrays) + len(moves): len(moves)} if grown else {},
        compiler_params=pltpu.CompilerParams(vmem_limit_bytes=67043328),
        cost_estimate=cost(size),
    )(*arrays, *moves, *((into,) if grown else ()))
    return out if moves else out[0]


def fresh_kernel(*refs):
    m, v, g, factor_ref, m_new, v_new = refs[:3], refs[3:6], refs[6:9], refs[9], refs[10:13], refs[13:16]
    bufs, in_s, out_s = refs[16:25], refs[25], refs[26]
    pieces = []
    for i in range(3):
        layers, height = m[i].shape[:2]
        pieces += [(i, layer, p * (height // 2), height // 2) for layer in range(layers) for p in range(2)]

    def loads(z):
        i, layer, r0, nr = pieces[z]
        at_rows = pl.ds(r0, nr)
        return [pltpu.make_async_copy(a[i].at[layer, at_rows], bufs[3 * t + i].at[layer, at_rows], in_s.at[t, z]) for t, a in enumerate((m, v, g))]

    def stores(z):
        i, layer, r0, nr = pieces[z]
        at_rows = pl.ds(r0, nr)
        return [pltpu.make_async_copy(bufs[3 * t + i].at[layer, at_rows], a[i].at[layer, at_rows], out_s.at[t, i]) for t, a in enumerate((m_new, v_new))]

    for z in range(len(pieces)):
        for copy in loads(z):
            copy.start()
    for z, (i, layer, r0, nr) in enumerate(pieces):
        for copy in loads(z):
            copy.wait()
        mm, vv, gg = (bufs[3 * t + i].at[layer] for t in range(3))
        tile = 65536 // mm.shape[1]

        def body(r, _, mm=mm, vv=vv, gg=gg, r0=r0, tile=tile):
            at_rows = pl.ds(pl.multiple_of(r0 + r * tile, tile), tile)
            grad = gg[at_rows, :].astype(F32) * factor_ref[0:1, 0:1]
            mm[at_rows, :], vv[at_rows, :] = moments(mm[at_rows, :], vv[at_rows, :], grad)
            return 0

        lax.fori_loop(0, nr // tile, body, 0)
        for copy in stores(z):
            copy.start()
    for t, arrays in enumerate((m_new, v_new)):
        for i in range(3):
            pltpu.make_async_copy(bufs[3 * t + i], arrays[i], out_s.at[t, i]).wait()


def fresh(m, v, sums, factor):
    pieces = 2 * sum(one.shape[0] for one in m)
    size = sum(one.size * 18 for one in m)
    dma = pltpu.SemaphoreType.DMA
    any_space = pl.BlockSpec(memory_space=pltpu.HBM)
    out = pl.pallas_call(
        fresh_kernel,
        name="fresh",
        out_shape=[jax.ShapeDtypeStruct(one.shape, F32) for one in (*m, *v)],
        in_specs=[any_space] * 9 + [pl.BlockSpec(memory_space=pltpu.VMEM)],
        out_specs=[any_space] * 6,
        scratch_shapes=[pltpu.VMEM(one.shape, one.dtype) for one in (*m, *v, *sums)] + [dma((3, pieces)), dma((2, 3))],
        compiler_params=pltpu.CompilerParams(vmem_limit_bytes=67043328),
        cost_estimate=cost(size),
    )(*m, *v, *sums, factor)
    return out[:3], out[3:]


def solution(mesh):
    n = mesh.shape["dp"]

    def step(*arrays):
        terms, weights, m, v = (arrays[i : i + 3] for i in (0, 3, 6, 9))
        layers = weights[0].shape[0]
        blocks = [(one.shape[1] // 2, one.shape[2]) for one in m]
        kinds = (blocks[0], blocks[2])
        count = float(n * sum(one.size for one in m))
        dma = pltpu.SemaphoreType.DMA
        units = [(i, layer) for i in range(3) for layer in range(layers)]
        halves = [b[0] for b in blocks]
        steps = rs_steps(units, halves)
        pieces = sum(units[piece[0]][0] < KEPT for piece in make_order(units, halves))
        swaps = max(len(exchange_list(steps, halves, units)), pieces + 6 * KEPT * layers)
        hops = max(sum(one.send for one in steps), 2 * pieces + 2 * KEPT * layers)
        any_space = pl.BlockSpec(memory_space=pl.ANY)
        half, cols = blocks[KEPT]
        tail = half // CUT
        shapes = [one.shape for one in weights[:KEPT]] + [(layers, half, cols)] * 4 + [(layers, half - tail, cols)] * 2 + [(layers, tail, cols)] * 2
        shapes += [one.shape for one in m]
        out = pl.pallas_call(
            functools.partial(kernel, n=n, layers=layers, count=count),
            name="step",
            out_shape=[jax.ShapeDtypeStruct(shape, BF) for shape in shapes] + [jax.ShapeDtypeStruct((8, 128), F32)],
            in_specs=[any_space] * 12,
            out_specs=[any_space] * (len(shapes) + 1),
            scratch_shapes=[pltpu.VMEM((4, layers, 2 * b[0], b[1]), BF) for b in blocks]
            + [pltpu.VMEM((6, layers, *b), BF) for b in blocks]
            + [pltpu.VMEM((RING, *b), BF) for b in kinds]
            + [pltpu.VMEM((size, *b), F32) for size, b in zip(FEED, kinds, strict=True)] * 2
            + [pltpu.VMEM((size, *b), BF) for size, b in zip(FEED, kinds, strict=True)]
            + [pltpu.VMEM((n + 1, 8, 128), F32), pltpu.VMEM((8, 128), F32)]
            + [dma((3,)), dma((swaps,)), dma((3,)), dma((hops,)), dma((2, RING)), dma((3, 2, max(FEED)))]
            + [dma((2,)), dma((3, KEPT)), dma((2, KEPT)), dma((3, KEPT)), dma((4, 3)), dma((2, 2)), dma((2, 2))],
            compiler_params=pltpu.CompilerParams(collective_id=0, has_side_effects=True, vmem_limit_bytes=67043328),
        )(*terms, *weights, *m, *v)
        kept, (low, high), (m_low, m_high), (low_a, high_a), (x_low_b, y_high_b) = (out[i : i + 2] for i in range(0, 10, 2))
        sums, factor = out[10:13], out[13]

        def hop(a, flip):
            return lax.ppermute(a, "dp", [(i, i ^ flip) for i in range(n)])

        barrier = lax.optimization_barrier
        x, y, mate = n // 2, n // 4, 1
        x_low_a, y_high_a = hop(low_a, x), hop(high_a, y)
        x_high, y_low = hop(high, x), hop(low, y)
        mx_b, my_b = hop(x_low_b, mate), hop(y_high_b, mate)
        new_m, new_v = fresh(m, v, sums, factor)
        x_low_a, y_high_a, new_m, new_v = barrier((x_low_a, y_high_a, new_m, new_v))
        d_low_a, d_high_a = hop(x_low_a, y), hop(y_high_a, x)
        d_low_b, d_high_b = hop(x_low_b, y), hop(y_high_b, x)
        mx_a, my_a = hop(x_low_a, mate), hop(y_high_a, mate)
        shape, b = weights[KEPT].shape, half - tail
        first = [((ME, 0, 0, 0), low), ((ME, 0, 1, 0), high), ((ME, 1, 0, 0), m_low), ((ME, 1, 1, 0), m_high)]
        first += [((XN, 0, 0, 0), x_low_a), ((YN, 0, 1, 0), y_high_a), ((XN, 0, 0, b), x_low_b), ((YN, 0, 1, b), y_high_b)]
        first += [((XN, 1, 0, b), mx_b), ((YN, 1, 1, b), my_b)]
        gate, up, down = place(first, shape, half, moves=kept)
        x_high, y_low, gate, up, down = barrier((x_high, y_low, gate, up, down))
        mx_high, my_low = hop(x_high, mate), hop(y_low, mate)
        then = [((XN, 1, 0, 0), mx_a), ((YN, 1, 1, 0), my_a), ((XN, 0, 1, 0), x_high), ((YN, 0, 0, 0), y_low)]
        down = place(then, shape, half, down)
        d_low_a, d_high_a, down = barrier((d_low_a, d_high_a, down))
        md_low_a, md_high_a = hop(d_low_a, mate), hop(d_high_a, mate)
        more = [((XN, 1, 1, 0), mx_high), ((YN, 1, 0, 0), my_low), ((DG, 0, 0, 0), d_low_a), ((DG, 0, 1, 0), d_high_a)]
        down = place(more, shape, half, down)
        d_low_b, d_high_b, down = barrier((d_low_b, d_high_b, down))
        md_low_b, md_high_b = hop(d_low_b, mate), hop(d_high_b, mate)
        down = place([((DG, 1, 0, 0), md_low_a), ((DG, 1, 1, 0), md_high_a)], shape, half, down)
        late_b = [((DG, 0, 0, b), d_low_b), ((DG, 0, 1, b), d_high_b), ((DG, 1, 0, b), md_low_b), ((DG, 1, 1, b), md_high_b)]
        down = place(late_b, shape, half, down)
        return (gate, up, down, *new_m, *new_v)

    all_of, cut = P(None, None, None), P(None, "dp", None)
    return jax.shard_map(
        step,
        mesh=mesh,
        in_specs=(P(("rep", "dp"), None, None, None),) * 3 + (all_of,) * 3 + (cut,) * 6,
        out_specs=(P("rep", None, None),) * 3 + (P("rep", "dp", None),) * 6,
        check_vma=False,
    )
```
